32 devices in a mesh: graph: 2 (over x), col: 4 (over z), row: 4 (over y, core).
Axes of the slice: x: 2, y: 2, z: 4, core: 2. Of those that a mesh axis runs over, the one named last changes fastest.
Arguments:
- flow_init: float32 [16384, 8192], P(('graph', 'row'), 'col'), parts along dimension 0
- flow_graph: float32 [16384, 8192], P(('graph', 'row'), 'col'), parts along dimension 0
Outputs:
- output: float32 [16384, 8192], P(('graph', 'row'), 'col'), parts along dimension 0
There are 2 independent parts. The reference program is written for one: setup_inputs(seed, part) draws one part's arguments, and reference() takes and returns one part's arrays. A program takes and returns all parts, laid end to end along the dimension named above; each array names one.
All inputs are finite; a program needn't handle non-finite values.
Results may differ from the reference program's by a relative error of at most 0.001.
Values are sent between devices in bfloat16 or wider.
A program may use at most 1 GiB of HBM per device.

```python
import jax
import jax.numpy as jnp
from jax import lax

N = 8192
ITERATIONS = 3


def draw_flow(key, floor_level):
    key_width, key_noise = jax.random.split(key)
    node_index = jnp.arange(N, dtype=jnp.float32)
    band_width = N * jax.random.uniform(key_width, (N,), minval=0.01, maxval=0.15)
    raw_offset = jnp.abs(node_index[:, None] - node_index[None, :])
    cyclic_dist = jnp.minimum(raw_offset, N - raw_offset)
    noise_fac = jax.random.uniform(key_noise, (N, N), minval=0.5, maxval=1.5)
    weight = (floor_level + jnp.exp(-cyclic_dist / band_width[None, :])) * noise_fac
    return weight / jnp.sum(weight, axis=0, keepdims=True)


def setup_inputs(seed: int = 0, part: int = 0) -> dict:
    key = jax.random.fold_in(jax.random.key(seed), part)
    key_init, key_graph = jax.random.split(key)
    flow_init = N * draw_flow(key_init, 0.05)
    flow_graph = draw_flow(key_graph, 0.1)
    return {"flow_init": flow_init.astype(jnp.float32), "flow_graph": flow_graph.astype(jnp.float32)}


def reference(flow_init, flow_graph):
    graph_bf = flow_graph.astype(jnp.bfloat16)

    def iteration(flow_cur, unused):
        expanded = jnp.dot(flow_cur.astype(jnp.bfloat16), graph_bf, preferred_element_type=jnp.float32)
        inflated = expanded * expanded
        col_sum = jnp.sum(inflated, axis=0)
        return inflated * (N / col_sum), None

    flow_out, _ = lax.scan(iteration, flow_init, None, length=ITERATIONS)
    return flow_out
```

```python
import functools

import jax
import jax.numpy as jnp
from jax import lax
from jax.experimental import pallas as pl
from jax.experimental.pallas import tpu as pltpu
from jax.sharding import PartitionSpec as P

ITERATIONS = 3
NQ = 8
MESH = pl.DeviceIdType.MESH
F32, BF16 = jnp.float32, jnp.bfloat16


def mcl_kernel(nb, mb, a_hbm, g_hbm, chome, gfull, abuf, A, C, gt, Sx, scale,
               ld_sem, st_sem, tl_sem, arecv, asend, grecv, zs, ys, ps, sr, ss, crecv, csend):
    tw = nb // NQ
    half = nb // 2
    order_n = 4 * nb
    z, i = lax.axis_index("col"), lax.axis_index("row")
    y, c = i // 2, i % 2
    side = z // 2
    mid, omid, end, oend = 1 + side, 2 - side, 3 * side, 3 - 3 * side
    is_mid = z == mid
    iy, ip = (1 - y) * 2 + c, y * 2 + (1 - c)
    iyp = (1 - y) * 2 + (1 - c)

    def rows(ii):
        return pl.ds(pl.multiple_of(ii * nb, nb), nb)

    def cols(q):
        return pl.ds(pl.multiple_of(q * tw, tw), tw)

    def halfrows(h):
        return pl.ds(pl.multiple_of(h * half, half), half)

    def gref(ii, tile):
        return gfull.at[tile, rows(ii), :]

    def gcopy(ii, tile, ssem, col, row):
        return pltpu.make_async_remote_copy(
            src_ref=gref(ii, tile), dst_ref=gref(ii, tile), send_sem=ssem, recv_sem=grecv.at[ii, tile],
            device_id={"col": col, "row": row}, device_id_type=MESH)

    def zcopy(ii, tile, s, q, col):
        return gcopy(ii, tile, zs.at[s, q], col, i)

    def ycopy(tile):
        return gcopy(i, tile, ys.at[tile], z, iy)

    def pcopy(ii, tile):
        return gcopy(ii, tile, ps.at[ii // 2, tile], z, ip)

    def gwait(ii, tile):
        gcopy(ii, tile, zs.at[0, 0], z, i).wait_recv()

    def loads(src, base, q, h):
        return pltpu.make_async_copy(src.at[halfrows(h), cols(q)], C.at[base + 2 * q + h], ld_sem.at[base + 2 * q + h])

    def each(n, body):
        def step(k, carry):
            body(k)
            return carry
        lax.fori_loop(0, n, step, 0)

    def start_loads(q):
        for h in range(2):
            loads(a_hbm, 0, q, h).start()
            loads(g_hbm, 2 * NQ, q, h).start()
    each(NQ, start_loads)

    barrier = pltpu.get_barrier_semaphore()
    me16 = z * 4 + i

    def knock(d):
        other = lax.rem(me16 + 1 + d, 16)
        pl.semaphore_signal(barrier, inc=1, device_id={"col": other // 4, "row": other % 4}, device_id_type=MESH)
    each(15, knock)
    pl.semaphore_wait(barrier, 15)

    def a_remote(q, h):
        return pltpu.make_async_remote_copy(
            src_ref=abuf.at[q, halfrows(h), :], dst_ref=A.at[:, cols(z * NQ + q)],
            send_sem=asend.at[h, q], recv_sem=arecv.at[z, q], device_id={"col": 1 + h, "row": i}, device_id_type=MESH)

    def a_local(q, h):
        return pltpu.make_async_copy(abuf.at[q, halfrows(h), :], A.at[:, cols(z * NQ + q)], arecv.at[z, q])

    def cast(src, base, q, dst):
        for h in range(2):
            loads(src, base, q, h).wait()
            gt[0, h * half:(h + 1) * half, :] = C[base + 2 * q + h].astype(BF16)
        put = pltpu.make_async_copy(gt.at[0, pl.ds(0, nb), :], dst, st_sem)
        put.start()
        put.wait()

    def hand_out(q):
        cast(a_hbm, 0, q, abuf.at[q])
        for h in range(2):
            @pl.when(z == 1 + h)
            def _():
                a_local(q, h).start()

            @pl.when(z != 1 + h)
            def _():
                a_remote(q, h).start()
        tile = z * NQ + q
        cast(g_hbm, 2 * NQ, q, gref(i, tile))
        ycopy(tile).start()

        @pl.when(is_mid)
        def _():
            pcopy(i, tile).start()
    each(NQ, hand_out)

    @pl.when(jnp.logical_not(is_mid))
    def _():
        def relay(q):
            tile = z * NQ + q
            zcopy(i, tile, 0, q, mid).start()
            gwait(iy, tile)
            zcopy(iy, tile, 1, q, mid).start()
        each(NQ, relay)

    def mtile(t):
        return jnp.where(t < NQ, omid * NQ + t, oend * NQ + t - NQ)

    def pump(t):
        @pl.when(t < 2 * NQ)
        def _():
            tm = mtile(t)
            gwait(i, tm)
            ycopy(tm).start()
            pcopy(i, tm).start()
            te = end * NQ + t // 2
            odd = t % 2

            @pl.when(odd == 0)
            def _():
                gwait(i, te)
                zcopy(i, te, 1, t // 2, omid).start()
                pcopy(i, te).start()

            @pl.when(odd == 1)
            def _():
                gwait(iy, te)
                pcopy(iy, te).start()

        @pl.when(jnp.logical_and(t >= 1, t <= 2 * NQ))
        def _():
            tm = mtile(t - 1)
            gwait(iy, tm)
            pcopy(iy, tm).start()

    me8 = (z - 1) * 4 + i

    def tile_load(tile, slot):
        return pltpu.make_async_copy(gfull.at[tile], gt.at[slot], tl_sem.at[slot])

    def compute(tile, slot, sx_slot):
        def block(m, s):
            r = pl.ds(pl.multiple_of(m * mb, mb), mb)
            acc = jnp.dot(A[r, :], gt[slot], preferred_element_type=F32)
            sq = acc * acc
            C[tile, r, :] = sq
            return s + jnp.sum(sq.reshape(mb // 8, 8, tw), axis=0)
        s = lax.fori_loop(0, half // mb, block, jnp.zeros((8, tw), F32))
        Sx[sx_slot, me8, :, cols(tile)] = jnp.sum(s, axis=0, keepdims=True)

    def s_copy(it, d):
        other = lax.rem(me8 + d, 8)
        return pltpu.make_async_remote_copy(
            src_ref=Sx.at[it, me8], dst_ref=Sx.at[it, me8], send_sem=ss.at[it, d], recv_sem=sr.at[it, me8],
            device_id={"col": 1 + other // 4, "row": other % 4}, device_id_type=MESH)

    def s_wait(it, src):
        pltpu.make_async_remote_copy(
            src_ref=Sx.at[it, src], dst_ref=Sx.at[it, src], send_sem=ss.at[it, 0], recv_sem=sr.at[it, src],
            device_id={"col": z, "row": i}, device_id_type=MESH).wait_recv()

    def renormalise(it):
        each(7, lambda d: s_copy(it, d + 1).start())
        each(7, lambda d: s_wait(it, lax.rem(me8 + d + 1, 8)))
        total = Sx[it, 0]
        for k in range(1, 8):
            total = total + Sx[it, k]
        scale[...] = float(order_n) / total

        def one(tile):
            fac = scale[:, cols(tile)]

            def part(m):
                r = pl.ds(pl.multiple_of(m * mb, mb), mb)
                A[r, cols(tile)] = (C[tile, r, :] * fac).astype(BF16)
            each(half // mb, part)
        each(4 * NQ, one)
        each(7, lambda d: s_copy(it, d + 1).wait_send())

    def order3(k):
        j = k - NQ
        both = jnp.where(j % 2 == 0, omid, end) * NQ + j // 2
        return jnp.where(k < NQ, oend * NQ + k, jnp.where(k < 3 * NQ, both, mid * NQ + k - 3 * NQ))

    def c_remote(tile):
        q = tile % NQ
        return pltpu.make_async_remote_copy(
            src_ref=C.at[tile], dst_ref=chome.at[halfrows(z - 1), cols(q)],
            send_sem=csend.at[tile], recv_sem=crecv.at[z - 1, q],
            device_id={"col": tile // NQ, "row": i}, device_id_type=MESH)

    def c_local(tile):
        q = tile % NQ
        return pltpu.make_async_copy(C.at[tile], chome.at[halfrows(z - 1), cols(q)], crecv.at[z - 1, q])

    def c_wait(h, q):
        pltpu.make_async_copy(chome.at[halfrows(h), cols(q)], chome.at[halfrows(h), cols(q)], crecv.at[h, q]).wait()

    @pl.when(is_mid)
    def _():
        def own_z(q):
            zcopy(i, z * NQ + q, 0, q, omid).start()
        each(NQ, own_z)

        def own_y(q):
            tile = z * NQ + q
            gwait(iy, tile)
            pcopy(iy, tile).start()
        each(NQ, own_y)

        def a_wait(k):
            zz, q = k // NQ, k % NQ
            pltpu.make_async_copy(abuf.at[q, halfrows(0), :], A.at[:, cols(k)], arecv.at[zz, q]).wait()
        each(4 * NQ, a_wait)

        def first(k):
            j = k - NQ
            p, r = j // 3, j % 3

            @pl.when(k == NQ // 2)
            def _():
                pump(0)

            @pl.when(k == NQ - 1)
            def _():
                pump(1)

            @pl.when(jnp.logical_and(k >= NQ, r != 1))
            def _():
                pump(2 * p + 2 + r // 2)
            tile = jnp.where(k < NQ, mid * NQ + k, jnp.where(r == 1, end * NQ + p, mtile(2 * p + r // 2)))
            gwait(ip, tile)
            gwait(iyp, tile)
            tile_load(tile, 0).start()
            tile_load(tile, 0).wait()
            compute(tile, 0, 0)
        each(4 * NQ, first)
        renormalise(0)

        def later(it):
            tile_load(order3(0), 0).start()

            def step(k):
                slot = k % 2
                tile = order3(k)
                tile_load(tile, slot).wait()

                @pl.when(k + 1 < 4 * NQ)
                def _():
                    tile_load(order3(k + 1), 1 - slot).start()
                compute(tile, slot, 1)

                @pl.when(it == 1)
                def _():
                    @pl.when(tile // NQ == z)
                    def _():
                        c_local(tile).start()

                    @pl.when(tile // NQ != z)
                    def _():
                        c_remote(tile).start()
            each(4 * NQ, step)

            @pl.when(it == 0)
            def _():
                renormalise(1)
        each(2, later)

    each(2 * NQ, lambda k: c_wait(k // NQ, k % NQ))

    def drain(q):
        tile = z * NQ + q
        ycopy(tile).wait_send()
        for h in range(2):
            @pl.when(z != 1 + h)
            def _():
                a_remote(q, h).wait_send()

        @pl.when(jnp.logical_not(is_mid))
        def _():
            zcopy(i, tile, 0, q, mid).wait_send()
            zcopy(iy, tile, 1, q, mid).wait_send()

        @pl.when(is_mid)
        def _():
            zcopy(i, tile, 0, q, omid).wait_send()
            zcopy(i, end * NQ + q, 1, q, omid).wait_send()
            ycopy(omid * NQ + q).wait_send()
            ycopy(oend * NQ + q).wait_send()
            for zz in range(4):
                pcopy(i, zz * NQ + q).wait_send()
                pcopy(iy, zz * NQ + q).wait_send()

                @pl.when(zz != z)
                def _():
                    c_remote(zz * NQ + q).wait_send()
    each(NQ, drain)


def solution(mesh):
    block_spec = P(("graph", "row"), "col")

    def device_step(init_blk, graph_blk):
        nb = init_blk.shape[1]
        n, tw = 4 * nb, nb // NQ
        mb = min(512, nb // 2)
        dma = pltpu.SemaphoreType.DMA
        any_spec = pl.BlockSpec(memory_space=pl.ANY)
        m_home, _, _ = pl.pallas_call(
            functools.partial(mcl_kernel, nb, mb),
            out_shape=(
                jax.ShapeDtypeStruct((nb, nb), F32),
                jax.ShapeDtypeStruct((4 * NQ, n, tw), BF16),
                jax.ShapeDtypeStruct((NQ, nb, tw), BF16),
            ),
            in_specs=[any_spec] * 2,
            out_specs=[any_spec] * 3,
            scratch_shapes=[
                pltpu.VMEM((nb // 2, n), BF16),
                pltpu.VMEM((4 * NQ, nb // 2, tw), F32),
                pltpu.VMEM((2, n, tw), BF16),
                pltpu.VMEM((2, 8, 1, n), F32),
                pltpu.VMEM((1, n), F32),
                dma((4 * NQ,)),
                dma(()),
                dma((2,)),
                dma((4, NQ)),
                dma((2, NQ)),
                dma((4, 4 * NQ)),
                dma((2, NQ)),
                dma((4 * NQ,)),
                dma((2, 4 * NQ)),
                dma((2, 8)),
                dma((2, 8)),
                dma((2, NQ)),
                dma((4 * NQ,)),
            ],
            compiler_params=pltpu.CompilerParams(
                collective_id=0, has_side_effects=True, vmem_limit_bytes=67043328),
            name="mcl",
        )(init_blk, graph_blk)
        col_sum = lax.psum(jnp.sum(m_home, axis=0), "row")
        return m_home * (n / col_sum)

    return jax.shard_map(device_step, mesh=mesh, in_specs=(block_spec, block_spec), out_specs=block_spec, check_vma=False)
```

```python
import functools

import jax
import jax.numpy as jnp
from jax import lax
from jax.experimental import pallas as pl
from jax.experimental.pallas import tpu as pltpu
from jax.sharding import PartitionSpec as P

ITERATIONS = 3
NQ = 8
NS = 2
MESH = pl.DeviceIdType.MESH
F32, BF16 = jnp.float32, jnp.bfloat16


def mcl_kernel(nb, mb, a_hbm, g_hbm, chome, shome, gfull, abuf, m1b, AA, C, gt, st, Sx, scale,
               ld_sem, put_sem, tl_sem, st_sem, arecv, asend, grecv, zs, ys, ps, sr, ss, crecv, csend, hrecv, hsend):
    tw = nb // NQ
    half = nb // 2
    sub = nb // NS
    order_n = 4 * nb
    z, i = lax.axis_index("col"), lax.axis_index("row")
    y, c = i // 2, i % 2
    side = z // 2
    mid, omid, end, oend = 1 + side, 2 - side, 3 * side, 3 - 3 * side
    is_mid = z == mid
    iy, ip = (1 - y) * 2 + c, y * 2 + (1 - c)
    iyp = (1 - y) * 2 + (1 - c)

    def pos(zz):
        return jnp.where(zz == 0, 2, jnp.where(zz == 3, 3, zz - 1))

    def spos(tile):
        return pos(tile // NQ) * NQ + tile % NQ

    def cols(q):
        return pl.ds(pl.multiple_of(q * tw, tw), tw)

    def halfrows(h):
        return pl.ds(pl.multiple_of(h * half, half), half)

    def gref(ii, tile, s):
        return gfull.at[tile, pl.ds(pl.multiple_of(pos(ii) * nb + s * sub, sub), sub), :]

    def gcopy(ii, tile, s, ssem, col, row):
        return pltpu.make_async_remote_copy(
            src_ref=gref(ii, tile, s), dst_ref=gref(ii, tile, s), send_sem=ssem, recv_sem=grecv.at[ii, tile, s],
            device_id={"col": col, "row": row}, device_id_type=MESH)

    def zcopy(ii, tile, s, k, q, col):
        return gcopy(ii, tile, s, zs.at[k, q, s], col, i)

    def ycopy(tile, s):
        return gcopy(i, tile, s, ys.at[tile, s], z, iy)

    def pcopy(ii, tile, s):
        return gcopy(ii, tile, s, ps.at[ii // 2, tile, s], z, ip)

    def gwait(ii, tile, s):
        gcopy(ii, tile, s, zs.at[0, 0, 0], z, i).wait_recv()

    def loads(src, base, q, h):
        return pltpu.make_async_copy(src.at[halfrows(h), cols(q)], C.at[base + 2 * q + h], ld_sem.at[base + 2 * q + h])

    def each(n, body):
        def step(k, carry):
            body(k)
            return carry
        lax.fori_loop(0, n, step, 0)

    def start_loads(q):
        for h in range(2):
            loads(a_hbm, 0, q, h).start()
            loads(g_hbm, 2 * NQ, q, h).start()
    each(NQ, start_loads)

    barrier = pltpu.get_barrier_semaphore()
    me16 = z * 4 + i

    def knock(d):
        other = lax.rem(me16 + 1 + d, 16)
        pl.semaphore_signal(barrier, inc=1, device_id={"col": other // 4, "row": other % 4}, device_id_type=MESH)
    each(15, knock)
    pl.semaphore_wait(barrier, 15)

    def a_dst(zz, q):
        return AA.at[pos(zz) // 2, :, cols(pos(zz) % 2 * NQ + q)]

    def a_remote(q, h):
        return pltpu.make_async_remote_copy(
            src_ref=abuf.at[q, halfrows(h), :], dst_ref=a_dst(z, q),
            send_sem=asend.at[h, q], recv_sem=arecv.at[z, q], device_id={"col": 1 + h, "row": i}, device_id_type=MESH)

    def a_local(q, h):
        return pltpu.make_async_copy(abuf.at[q, halfrows(h), :], a_dst(z, q), arecv.at[z, q])

    def cast(src, base, q, dst):
        for h in range(2):
            loads(src, base, q, h).wait()
            gt[0, h * half:(h + 1) * half, :] = C[base + 2 * q + h].astype(BF16)
        put = pltpu.make_async_copy(gt.at[0, pl.ds(0, nb), :], dst, put_sem)
        put.start()
        put.wait()

    def hand_out(q):
        cast(a_hbm, 0, q, abuf.at[q])
        for h in range(2):
            @pl.when(z == 1 + h)
            def _():
                a_local(q, h).start()

            @pl.when(z != 1 + h)
            def _():
                a_remote(q, h).start()
        tile = z * NQ + q
        cast(g_hbm, 2 * NQ, q, gfull.at[tile, pl.ds(pl.multiple_of(pos(i) * nb, nb), nb), :])
        for s in range(NS):
            ycopy(tile, s).start()

            @pl.when(is_mid)
            def _():
                pcopy(i, tile, s).start()
    each(NQ, hand_out)

    @pl.when(jnp.logical_not(is_mid))
    def _():
        def relay(q):
            tile = z * NQ + q
            for s in range(NS):
                zcopy(i, tile, s, 0, q, mid).start()
            for s in range(NS):
                gwait(iy, tile, s)
                zcopy(iy, tile, s, 1, q, mid).start()
        each(NQ, relay)

    def mtile(t):
        return jnp.where(t < NQ, omid * NQ + t, oend * NQ + t - NQ)

    def pump(t):
        @pl.when(t < 2 * NQ)
        def _():
            tm = mtile(t)
            for s in range(NS):
                gwait(i, tm, s)
                ycopy(tm, s).start()
                pcopy(i, tm, s).start()
            te = end * NQ + t // 2
            odd = t % 2

            @pl.when(odd == 0)
            def _():
                for s in range(NS):
                    gwait(i, te, s)
                    zcopy(i, te, s, 1, t // 2, omid).start()
                    pcopy(i, te, s).start()

            @pl.when(odd == 1)
            def _():
                for s in range(NS):
                    gwait(iy, te, s)
                    pcopy(iy, te, s).start()

        @pl.when(jnp.logical_and(t >= 1, t <= 2 * NQ))
        def _():
            tm = mtile(t - 1)
            for s in range(NS):
                gwait(iy, tm, s)
                pcopy(iy, tm, s).start()

    me8 = (z - 1) * 4 + i

    def half_load(tile, k, slot):
        return pltpu.make_async_copy(
            gfull.at[tile, pl.ds(pl.multiple_of(k * 2 * nb, 2 * nb), 2 * nb), :], gt.at[slot], tl_sem.at[slot])

    def blocks(body):
        def step(m, s):
            return body(pl.ds(pl.multiple_of(m * mb, mb), mb), s)
        return lax.fori_loop(0, half // mb, step, jnp.zeros((8, tw), F32))

    def fold(sq):
        return jnp.sum(sq.reshape(mb // 8, 8, tw), axis=0)

    def put_sum(it, tile, s):
        Sx[it, me8, :, cols(spos(tile))] = jnp.sum(s, axis=0, keepdims=True)

    def full(it, tile, dst):
        def block(r, s):
            acc = jnp.dot(AA[0, r, :], gt[0], preferred_element_type=F32)
            acc = acc + jnp.dot(AA[1, r, :], gt[1], preferred_element_type=F32)
            sq = acc * acc
            dst[r, :] = sq
            return s + fold(sq)
        put_sum(it, tile, blocks(block))

    def first_half(tile, slot):
        def block(r, s):
            C[tile, r, :] = jnp.dot(AA[2, r, :], gt[slot], preferred_element_type=F32)
            return s
        blocks(block)

    def second_half(tile, slot):
        def block(r, s):
            acc = C[tile, r, :] + jnp.dot(AA[1, r, :], gt[slot], preferred_element_type=F32)
            sq = acc * acc
            C[tile, r, :] = sq
            return s + fold(sq)
        put_sum(1, tile, blocks(block))

    def s_copy(part, src, d):
        other = lax.rem(me8 + d, 8)
        if part < 2:
            ref = Sx.at[0, src, :, pl.ds(part * 2 * nb, 2 * nb)]
        else:
            ref = Sx.at[1, src]
        return pltpu.make_async_remote_copy(
            src_ref=ref, dst_ref=ref, send_sem=ss.at[part, d], recv_sem=sr.at[part, src],
            device_id={"col": 1 + other // 4, "row": other % 4}, device_id_type=MESH)

    def sums(part):
        each(7, lambda d: s_copy(part, me8, d + 1).start())
        each(7, lambda d: s_copy(part, lax.rem(me8 + d + 1, 8), 0).wait_recv())
        lo, n, it = (part * 2 * nb, 2 * nb, 0) if part < 2 else (0, 4 * nb, 1)
        total = Sx[it, 0, :, lo:lo + n]
        for k in range(1, 8):
            total = total + Sx[it, k, :, lo:lo + n]
        scale[:, lo:lo + n] = float(order_n) / total
        each(7, lambda d: s_copy(part, me8, d + 1).wait_send())

    def renorm(src, p, buf):
        fac = scale[:, cols(p)]

        def part(m):
            r = pl.ds(pl.multiple_of(m * mb, mb), mb)
            AA[buf, r, cols(p % (2 * NQ))] = (src[r, :] * fac).astype(BF16)
        each(half // mb, part)

    def m1_put(slot, k):
        return pltpu.make_async_copy(st.at[slot], m1b.at[k], st_sem.at[slot])

    def m1_get(slot, k):
        return pltpu.make_async_copy(m1b.at[k], st.at[slot], st_sem.at[slot])

    def order3(k):
        j = k - NQ
        both = jnp.where(j % 2 == 0, omid, end) * NQ + j // 2
        return jnp.where(k < NQ, oend * NQ + k, jnp.where(k < 3 * NQ, both, mid * NQ + k - 3 * NQ))

    def c_remote(tile):
        q = tile % NQ
        return pltpu.make_async_remote_copy(
            src_ref=C.at[tile], dst_ref=chome.at[halfrows(z - 1), cols(q)],
            send_sem=csend.at[tile], recv_sem=crecv.at[z - 1, q],
            device_id={"col": tile // NQ, "row": i}, device_id_type=MESH)

    def c_local(tile):
        q = tile % NQ
        return pltpu.make_async_copy(C.at[tile], chome.at[halfrows(z - 1), cols(q)], crecv.at[z - 1, q])

    def c_wait(h, q):
        pltpu.make_async_copy(chome.at[halfrows(h), cols(q)], chome.at[halfrows(h), cols(q)], crecv.at[h, q]).wait()

    def home_sum(k):
        zz, ii = k // 4, k % 4
        return pltpu.make_async_remote_copy(
            src_ref=Sx.at[2, me8, :, pl.ds(pl.multiple_of(pos(zz) * nb, nb), nb)], dst_ref=shome.at[me8],
            send_sem=hsend.at[k], recv_sem=hrecv.at[me8],
            device_id={"col": zz, "row": ii}, device_id_type=MESH)

    def home_sum_local():
        return pltpu.make_async_copy(
            Sx.at[2, me8, :, pl.ds(pl.multiple_of(pos(z) * nb, nb), nb)], shome.at[me8], hrecv.at[me8])

    @pl.when(is_mid)
    def _():
        def own_z(q):
            for s in range(NS):
                zcopy(i, z * NQ + q, s, 0, q, omid).start()
        each(NQ, own_z)

        def own_y(q):
            tile = z * NQ + q
            for s in range(NS):
                gwait(iy, tile, s)
                pcopy(iy, tile, s).start()
        each(NQ, own_y)

        def a_wait(k):
            zz, q = k // NQ, k % NQ
            pltpu.make_async_copy(abuf.at[q, halfrows(0), :], a_dst(zz, q), arecv.at[zz, q]).wait()
        each(4 * NQ, a_wait)

        def fetch(tile):
            for s in range(NS):
                gwait(ip, tile, s)
                gwait(iyp, tile, s)
            for k in range(2):
                half_load(tile, k, k).start()
            for k in range(2):
                half_load(tile, k, k).wait()

        def own_cols(k):
            @pl.when(k == NQ // 2)
            def _():
                pump(0)

            @pl.when(k == NQ - 1)
            def _():
                pump(1)
            tile = mid * NQ + k
            fetch(tile)
            full(0, tile, C.at[tile])
        each(NQ, own_cols)

        def advance(p, r):
            @pl.when(jnp.logical_and(r != 1, jnp.logical_or(p < NQ - 1, r == 2)))
            def _():
                pump(jnp.where(p < NQ - 1, 2 * p + 2 + r // 2, 2 * NQ))

        def tile_of(p, r):
            return jnp.where(r == 1, end * NQ + p, mtile(2 * p + r // 2))

        def b_number(tile):
            return jnp.where(tile // NQ == end, tile % NQ, NQ + tile % NQ)

        def to_stage(n, tile):
            slot = n % 2

            @pl.when(n >= 2)
            def _():
                m1_put(slot, 0).wait()
            full(0, tile, st.at[slot])
            m1_put(slot, b_number(tile)).start()

        def early(k):
            p, r = k // 3, k % 3
            advance(p, r)
            tile = tile_of(p, r)
            fetch(tile)

            @pl.when(r == 1)
            def _():
                to_stage(p, tile)

            @pl.when(r != 1)
            def _():
                full(0, tile, C.at[tile])
        each(3 * NQ // 2, early)

        sums(0)

        def renorm_a(p):
            zz = 1 + p // NQ
            renorm(C.at[zz * NQ + p % NQ], p, 2)
        each(2 * NQ, renorm_a)

        def extra(e):
            return jnp.where(e < 2 * NQ, NQ + e, end * NQ + e - 2 * NQ)

        def rest(k):
            p, r = NQ // 2 + k // 3, k % 3
            advance(p, r)
            tile = tile_of(p, r)
            fetch(tile)
            to_stage(NQ // 2 + k, tile)
            more = k < 5 * NQ // 4

            @pl.when(more)
            def _():
                half_load(extra(2 * k), 0, 1).start()

            def three(u):
                slot = u % 2

                @pl.when(u > 0)
                def _():
                    half_load(0, 0, slot).wait()

                @pl.when(u == 1)
                def _():
                    half_load(extra(2 * k + 1), 0, 0).start()
                first_half(jnp.where(u == 0, tile, extra(2 * k + u - 1)), slot)
            lax.fori_loop(0, jnp.where(more, 3, 1), lambda u, x: (three(u), x)[1], 0)
        each(3 * NQ // 2, rest)
        half_load(0, 1, 0).start()
        half_load(NQ, 1, 1).start()
        for slot in range(2):
            m1_put(slot, 0).wait()

        def b_index(p):
            zz = jnp.where(p < NQ, 0, 3)
            return b_number(zz * NQ + p % NQ)

        for slot in range(2):
            m1_get(slot, b_index(slot)).start()
        sums(1)

        def renorm_b(p):
            slot = p % 2
            m1_get(slot, 0).wait()
            renorm(st.at[slot], 2 * NQ + p, 1)

            @pl.when(p + 2 < 2 * NQ)
            def _():
                m1_get(slot, b_index(p + 2)).start()
        each(2 * NQ, renorm_b)

        def order2(k):
            return (k % 4) * NQ + k // 4

        def second(k):
            slot = k % 2
            tile = order2(k)
            half_load(tile, 1, slot).wait()
            second_half(tile, slot)

            @pl.when(k + 2 < 4 * NQ)
            def _():
                half_load(order2(k + 2), 1, slot).start()
        each(4 * NQ, second)
        for k in range(2):
            half_load(order3(0), k, k).start()
        sums(2)

        def renorm_2(p):
            pz = p // NQ
            zz = jnp.where(pz == 2, 0, jnp.where(pz == 3, 3, pz + 1))
            renorm(C.at[zz * NQ + p % NQ], p, p // (2 * NQ))
        each(4 * NQ, renorm_2)

        def third(k):
            tile = order3(k)
            for u in range(2):
                half_load(tile, u, u).wait()
            full(2, tile, C.at[tile])

            @pl.when(k + 1 < 4 * NQ)
            def _():
                for u in range(2):
                    half_load(order3(k + 1), u, u).start()

            @pl.when(tile // NQ == z)
            def _():
                c_local(tile).start()

            @pl.when(tile // NQ != z)
            def _():
                c_remote(tile).start()
        each(4 * NQ, third)

        def send_sums(k):
            @pl.when(k == me16)
            def _():
                home_sum_local().start()

            @pl.when(k != me16)
            def _():
                home_sum(k).start()
        each(16, send_sums)

    each(2 * NQ, lambda k: c_wait(k // NQ, k % NQ))
    each(8, lambda m: pltpu.make_async_copy(shome.at[m], shome.at[m], hrecv.at[m]).wait())

    def drain(q):
        tile = z * NQ + q
        for h in range(2):
            @pl.when(z != 1 + h)
            def _():
                a_remote(q, h).wait_send()
        for s in range(NS):
            ycopy(tile, s).wait_send()

            @pl.when(jnp.logical_not(is_mid))
            def _():
                zcopy(i, tile, s, 0, q, mid).wait_send()
                zcopy(iy, tile, s, 1, q, mid).wait_send()

            @pl.when(is_mid)
            def _():
                zcopy(i, tile, s, 0, q, omid).wait_send()
                zcopy(i, end * NQ + q, s, 1, q, omid).wait_send()
                ycopy(omid * NQ + q, s).wait_send()
                ycopy(oend * NQ + q, s).wait_send()
                for zz in range(4):
                    pcopy(i, zz * NQ + q, s).wait_send()
                    pcopy(iy, zz * NQ + q, s).wait_send()

        @pl.when(is_mid)
        def _():
            for zz in range(4):
                @pl.when(zz != z)
                def _():
                    c_remote(zz * NQ + q).wait_send()
            for k in range(2):
                @pl.when(2 * q + k != me16)
                def _():
                    home_sum(2 * q + k).wait_send()
    each(NQ, drain)


def solution(mesh):
    block_spec = P(("graph", "row"), "col")

    def device_step(init_blk, graph_blk):
        nb = init_blk.shape[1]
        n, tw = 4 * nb, nb // NQ
        mb = min(512, nb // 2)
        dma = pltpu.SemaphoreType.DMA
        any_spec = pl.BlockSpec(memory_space=pl.ANY)
        m_home, s_home, _, _, _ = pl.pallas_call(
            functools.partial(mcl_kernel, nb, mb),
            out_shape=(
                jax.ShapeDtypeStruct((nb, nb), F32),
                jax.ShapeDtypeStruct((8, 1, nb), F32),
                jax.ShapeDtypeStruct((4 * NQ, n, tw), BF16),
                jax.ShapeDtypeStruct((NQ, nb, tw), BF16),
                jax.ShapeDtypeStruct((2 * NQ, nb // 2, tw), F32),
            ),
            in_specs=[any_spec] * 2,
            out_specs=[any_spec] * 5,
            scratch_shapes=[
                pltpu.VMEM((3, nb // 2, 2 * nb), BF16),
                pltpu.VMEM((4 * NQ, nb // 2, tw), F32),
                pltpu.VMEM((2, 2 * nb, tw), BF16),
                pltpu.VMEM((2, nb // 2, tw), F32),
                pltpu.VMEM((3, 8, 1, n), F32),
                pltpu.VMEM((1, n), F32),
                dma((4 * NQ,)),
                dma(()),
                dma((2,)),
                dma((2,)),
                dma((4, NQ)),
                dma((2, NQ)),
                dma((4, 4 * NQ, NS)),
                dma((2, NQ, NS)),
                dma((4 * NQ, NS)),
                dma((2, 4 * NQ, NS)),
                dma((3, 8)),
                dma((3, 8)),
                dma((2, NQ)),
                dma((4 * NQ,)),
                dma((8,)),
                dma((16,)),
            ],
            compiler_params=pltpu.CompilerParams(
                collective_id=0, has_side_effects=True, vmem_limit_bytes=67043328),
            name="mcl",
        )(init_blk, graph_blk)
        col_sum = jnp.sum(s_home, axis=(0, 1))
        return m_home * (n / col_sum)

    return jax.shard_map(device_step, mesh=mesh, in_specs=(block_spec, block_spec), out_specs=block_spec, check_vma=False)
```

```python
import functools

import jax
import jax.numpy as jnp
from jax import lax
from jax.experimental import pallas as pl
from jax.experimental.pallas import tpu as pltpu
from jax.sharding import PartitionSpec as P

ITERATIONS = 3
NQ = 8
NS = 2
MESH = pl.DeviceIdType.MESH
F32, BF16 = jnp.float32, jnp.bfloat16


def mcl_kernel(nb, mb, a_hbm, g_hbm, chome, shome, gfull, abuf, m1b, AA, C, gt, st, Sx, scale,
               ld_sem, put_sem, tl_sem, st_sem, arecv, asend, grecv, precv, zs, ys, ps, sr, ss, crecv, csend, hrecv, hsend):
    tw = nb // NQ
    half = nb // 2
    sub = nb // NS
    order_n = 4 * nb
    z, i = lax.axis_index("col"), lax.axis_index("row")
    y, c = i // 2, i % 2
    side = z // 2
    mid, omid, end, oend = 1 + side, 2 - side, 3 * side, 3 - 3 * side
    is_mid = z == mid
    iy, ip = (1 - y) * 2 + c, y * 2 + (1 - c)
    iyp = (1 - y) * 2 + (1 - c)

    def pos(zz):
        return jnp.where(zz == 0, 2, jnp.where(zz == 3, 3, zz - 1))

    def spos(tile):
        return pos(tile // NQ) * NQ + tile % NQ

    def cols(q):
        return pl.ds(pl.multiple_of(q * tw, tw), tw)

    def halfrows(h):
        return pl.ds(pl.multiple_of(h * half, half), half)

    def gref(ii, tile, s):
        return gfull.at[tile, pl.ds(pl.multiple_of(pos(ii) * nb + s * sub, sub), sub), :]

    def gcopy(ii, tile, s, ssem, rsem, col, row):
        return pltpu.make_async_remote_copy(
            src_ref=gref(ii, tile, s), dst_ref=gref(ii, tile, s), send_sem=ssem, recv_sem=rsem,
            device_id={"col": col, "row": row}, device_id_type=MESH)

    def zcopy(ii, tile, s, col):
        return gcopy(ii, tile, s, zs, grecv.at[ii // 2, tile, s], col, i)

    def ycopy(tile, s):
        return gcopy(i, tile, s, ys, grecv.at[i // 2, tile, s], z, iy)

    def pcopy(ii, tile, s):
        return gcopy(ii, tile, s, ps, precv.at[tile], z, ip)

    def done(ref, sem):
        pltpu.make_async_copy(ref, ref, sem).wait()

    def gwait(ii, tile, s):
        done(gref(ii, tile, s), grecv.at[ii // 2, tile, s])

    def loads(src, base, q, h):
        return pltpu.make_async_copy(src.at[halfrows(h), cols(q)], C.at[base + 2 * q + h], ld_sem.at[base // 2 + q])

    def each(n, body):
        def step(k, carry):
            body(k)
            return carry
        lax.fori_loop(0, n, step, 0)

    def start_loads(q):
        for h in range(2):
            loads(a_hbm, 0, q, h).start()
            loads(g_hbm, 2 * NQ, q, h).start()
    each(NQ, start_loads)

    barrier = pltpu.get_barrier_semaphore()
    me16 = z * 4 + i

    def knock(d):
        other = lax.rem(me16 + 1 + d, 16)
        pl.semaphore_signal(barrier, inc=1, device_id={"col": other // 4, "row": other % 4}, device_id_type=MESH)
    each(15, knock)
    pl.semaphore_wait(barrier, 15)

    def a_dst(zz, q):
        return AA.at[pos(zz) // 2, :, cols(pos(zz) % 2 * NQ + q)]

    def a_remote(q, h):
        return pltpu.make_async_remote_copy(
            src_ref=abuf.at[q, halfrows(h), :], dst_ref=a_dst(z, q),
            send_sem=asend, recv_sem=arecv, device_id={"col": 1 + h, "row": i}, device_id_type=MESH)

    def a_local(q, h):
        return pltpu.make_async_copy(abuf.at[q, halfrows(h), :], a_dst(z, q), arecv)

    def cast(src, base, q, dst):
        done(C.at[pl.ds(base + 2 * q, 2)], ld_sem.at[base // 2 + q])
        for h in range(2):
            gt[0, h * half:(h + 1) * half, :] = C[base + 2 * q + h].astype(BF16)
        put = pltpu.make_async_copy(gt.at[0, pl.ds(0, nb), :], dst, put_sem)
        put.start()
        put.wait()

    def hand_out(q):
        cast(a_hbm, 0, q, abuf.at[q])
        for h in range(2):
            @pl.when(z == 1 + h)
            def _():
                a_local(q, h).start()

            @pl.when(z != 1 + h)
            def _():
                a_remote(q, h).start()
        tile = z * NQ + q
        cast(g_hbm, 2 * NQ, q, gfull.at[tile, pl.ds(pl.multiple_of(pos(i) * nb, nb), nb), :])
        for s in range(NS):
            ycopy(tile, s).start()

            @pl.when(is_mid)
            def _():
                pcopy(i, tile, s).start()
    with jax.named_scope("hand_out"):
        each(NQ, hand_out)

    @pl.when(jnp.logical_not(is_mid))
    def _():
        def relay(q):
            tile = z * NQ + q
            for s in range(NS):
                zcopy(i, tile, s, mid).start()
            for s in range(NS):
                gwait(iy, tile, s)
                zcopy(iy, tile, s, mid).start()
        with jax.named_scope("relay"):
            each(NQ, relay)

    def mtile(t):
        return jnp.where(t < NQ, omid * NQ + t, oend * NQ + t - NQ)

    def own_z(q):
        for s in range(NS):
            zcopy(i, z * NQ + q, s, omid).start()

    def pump(t):
        @pl.when(t < 2 * NQ)
        def _():
            tm = mtile(t)
            for s in range(NS):
                gwait(i, tm, s)
                ycopy(tm, s).start()
                pcopy(i, tm, s).start()
            te = end * NQ + t // 2
            odd = t % 2

            @pl.when(odd == 0)
            def _():
                for s in range(NS):
                    gwait(i, te, s)
                    pcopy(i, te, s).start()

            @pl.when(odd == 1)
            def _():
                for s in range(NS):
                    gwait(iy, te, s)
                    pcopy(iy, te, s).start()

        @pl.when(t < NQ - 2)
        def _():
            own_z(t + 2)

        @pl.when(jnp.logical_or(jnp.logical_and(t >= NQ - 2, t <= 2 * NQ - 4), t == 2 * NQ - 2))
        def _():
            for s in range(NS):
                zcopy(i, end * NQ + jnp.minimum(t - NQ + 2, NQ - 1), s, omid).start()

        @pl.when(t >= 1)
        def _():
            tm = mtile(t - 1)
            for s in range(NS):
                gwait(iy, tm, s)
                pcopy(iy, tm, s).start()

    me8 = (z - 1) * 4 + i

    def half_load(tile, k, slot):
        return pltpu.make_async_copy(
            gfull.at[tile, pl.ds(pl.multiple_of(k * 2 * nb, 2 * nb), 2 * nb), :], gt.at[slot], tl_sem.at[slot])

    def blocks(body):
        def step(m, s):
            return body(pl.ds(pl.multiple_of(m * mb, mb), mb), s)
        return lax.fori_loop(0, half // mb, step, jnp.zeros((8, tw), F32))

    def fold(sq):
        return jnp.sum(sq.reshape(mb // 8, 8, tw), axis=0)

    def put_sum(it, tile, s):
        Sx[it, me8, :, cols(spos(tile))] = jnp.sum(s, axis=0, keepdims=True)

    def full(it, tile, dst):
        def block(r, s):
            acc = jnp.dot(AA[0, r, :], gt[0], preferred_element_type=F32)
            acc = acc + jnp.dot(AA[1, r, :], gt[1], preferred_element_type=F32)
            sq = acc * acc
            dst[r, :] = sq
            return s + fold(sq)
        put_sum(it, tile, blocks(block))

    def first_half(tile, slot):
        def block(r, s):
            C[tile, r, :] = jnp.dot(AA[2, r, :], gt[slot], preferred_element_type=F32)
            return s
        blocks(block)

    def second_half(tile, slot):
        def block(r, s):
            acc = C[tile, r, :] + jnp.dot(AA[1, r, :], gt[slot], preferred_element_type=F32)
            sq = acc * acc
            C[tile, r, :] = sq
            return s + fold(sq)
        put_sum(1, tile, blocks(block))

    def s_ref(part, src, n):
        if part < 2:
            return Sx.at[0, pl.ds(src, n), :, pl.ds(part * 2 * nb, 2 * nb)]
        return Sx.at[1, pl.ds(src, n)]

    def s_start(part):
        def send(d):
            other = lax.rem(me8 + d + 1, 8)
            pltpu.make_async_remote_copy(
                src_ref=s_ref(part, me8, 1), dst_ref=s_ref(part, me8, 1), send_sem=ss.at[part], recv_sem=sr.at[part],
                device_id={"col": 1 + other // 4, "row": other % 4}, device_id_type=MESH).start()
        each(7, send)

    def s_finish(part):
        done(s_ref(part, 0, 7), sr.at[part])
        lo, n, it = (part * 2 * nb, 2 * nb, 0) if part < 2 else (0, 4 * nb, 1)
        total = Sx[it, 0, :, lo:lo + n]
        for k in range(1, 8):
            total = total + Sx[it, k, :, lo:lo + n]
        scale[:, lo:lo + n] = float(order_n) / total
        done(s_ref(part, 0, 7), ss.at[part])

    def renorm(src, p, buf):
        fac = scale[:, cols(p)]

        def part(m):
            r = pl.ds(pl.multiple_of(m * mb, mb), mb)
            AA[buf, r, cols(p % (2 * NQ))] = (src[r, :] * fac).astype(BF16)
        each(half // mb, part)

    def m1_put(slot, k):
        return pltpu.make_async_copy(st.at[slot], m1b.at[k], st_sem.at[slot])

    def m1_get(slot, k):
        return pltpu.make_async_copy(m1b.at[k], st.at[slot], st_sem.at[slot])

    def order3(k):
        j = k - NQ
        both = jnp.where(j % 2 == 0, omid, end) * NQ + j // 2
        return jnp.where(k < NQ, oend * NQ + k, jnp.where(k < 3 * NQ, both, mid * NQ + k - 3 * NQ))

    def c_remote(tile):
        q = tile % NQ
        return pltpu.make_async_remote_copy(
            src_ref=C.at[tile], dst_ref=chome.at[halfrows(z - 1), cols(q)],
            send_sem=csend, recv_sem=crecv,
            device_id={"col": tile // NQ, "row": i}, device_id_type=MESH)

    def c_local(tile):
        q = tile % NQ
        return pltpu.make_async_copy(C.at[tile], chome.at[halfrows(z - 1), cols(q)], crecv)

    def home_sum(k):
        zz, ii = k // 4, k % 4
        return pltpu.make_async_remote_copy(
            src_ref=Sx.at[2, me8, :, pl.ds(pl.multiple_of(pos(zz) * nb, nb), nb)], dst_ref=shome.at[me8],
            send_sem=hsend.at[k], recv_sem=hrecv,
            device_id={"col": zz, "row": ii}, device_id_type=MESH)

    def home_sum_local():
        return pltpu.make_async_copy(
            Sx.at[2, me8, :, pl.ds(pl.multiple_of(pos(z) * nb, nb), nb)], shome.at[me8], hrecv)

    @pl.when(is_mid)
    def _():
        own_z(0)
        own_z(1)

        def own_y(q):
            tile = z * NQ + q
            for s in range(NS):
                gwait(iy, tile, s)
                pcopy(iy, tile, s).start()
        with jax.named_scope("own_y"):
            each(NQ, own_y)

        with jax.named_scope("a_wait"):
            done(AA.at[pl.ds(0, 2)], arecv)

        def fetch(tile):
            done(gfull.at[tile, pl.ds(0, 2 * nb), :], precv.at[tile])
            for k in range(2):
                half_load(tile, k, k).start()
            for k in range(2):
                half_load(tile, k, k).wait()

        def own_cols(k):
            @pl.when(k == NQ // 2)
            def _():
                pump(0)
            tile = mid * NQ + k
            with jax.named_scope("fetch"):
                fetch(tile)
            full(0, tile, C.at[tile])
        with jax.named_scope("own_cols"):
            each(NQ, own_cols)

        def advance(p, r):
            @pl.when(r != 1)
            def _():
                pump(2 * p + 1 + r // 2)

        def tile_of(p, r):
            return jnp.where(r == 1, end * NQ + p, mtile(2 * p + r // 2))

        def b_number(tile):
            return jnp.where(tile // NQ == end, tile % NQ, NQ + tile % NQ)

        def to_stage(n, tile):
            slot = n % 2

            @pl.when(n >= 2)
            def _():
                m1_put(slot, 0).wait()
            full(0, tile, st.at[slot])
            m1_put(slot, b_number(tile)).start()

        def early(k):
            p, r = k // 3, k % 3
            with jax.named_scope("advance"):
                advance(p, r)
            tile = tile_of(p, r)
            with jax.named_scope("fetch"):
                fetch(tile)

            @pl.when(r == 1)
            def _():
                to_stage(p, tile)

            @pl.when(r != 1)
            def _():
                full(0, tile, C.at[tile])
        with jax.named_scope("early"):
            each(3 * NQ // 2, early)

        s_start(0)

        def rest(k):
            p, r = NQ // 2 + k // 3, k % 3
            with jax.named_scope("advance"):
                advance(p, r)
            tile = tile_of(p, r)
            with jax.named_scope("fetch"):
                fetch(tile)
            to_stage(NQ // 2 + k, tile)
            return tile
        with jax.named_scope("rest3"):
            each(3, rest)
        with jax.named_scope("sums0"):
            s_finish(0)

        def renorm_a(p):
            zz = 1 + p // NQ
            renorm(C.at[zz * NQ + p % NQ], p, 2)
        with jax.named_scope("renorm_a"):
            each(2 * NQ, renorm_a)

        def extra(e):
            b = e - 2 * NQ
            return jnp.where(e < 2 * NQ, NQ + e, jnp.where(b < 5, end * NQ + b, oend * NQ + b - 5))

        def both(k):
            tile = rest(k + 3)
            more = jnp.where(k < 7, 3, jnp.where(k == 7, 2, 0))

            def part(u, carry):
                slot = u % 2

                @pl.when(u > 0)
                def _():
                    half_load(0, 0, slot).wait()

                @pl.when(u < more)
                def _():
                    half_load(extra(3 * k + u), 0, 1 - slot).start()
                first_half(jnp.where(u == 0, tile, extra(3 * k + u - 1)), slot)
                return carry
            lax.fori_loop(0, more + 1, part, 0)
        with jax.named_scope("both"):
            each(9, both)
        half_load(0, 1, 0).start()
        half_load(NQ, 1, 1).start()
        for slot in range(2):
            m1_put(slot, 0).wait()

        def b_index(p):
            zz = jnp.where(p < NQ, 0, 3)
            return b_number(zz * NQ + p % NQ)

        for slot in range(2):
            m1_get(slot, b_index(slot)).start()
        s_start(1)
        with jax.named_scope("sums1"):
            s_finish(1)

        def renorm_b(p):
            slot = p % 2
            m1_get(slot, 0).wait()
            renorm(st.at[slot], 2 * NQ + p, 1)

            @pl.when(p + 2 < 2 * NQ)
            def _():
                m1_get(slot, b_index(p + 2)).start()
        with jax.named_scope("renorm_b"):
            each(2 * NQ, renorm_b)

        def order2(k):
            return (k % 4) * NQ + k // 4

        def second(k):
            slot = k % 2
            tile = order2(k)
            half_load(tile, 1, slot).wait()
            second_half(tile, slot)

            @pl.when(k + 2 < 4 * NQ)
            def _():
                half_load(order2(k + 2), 1, slot).start()
        with jax.named_scope("second"):
            each(4 * NQ, second)
        for k in range(2):
            half_load(order3(0), k, k).start()
        s_start(2)
        with jax.named_scope("sums2"):
            s_finish(2)

        def renorm_2(p):
            pz = p // NQ
            zz = jnp.where(pz == 2, 0, jnp.where(pz == 3, 3, pz + 1))
            renorm(C.at[zz * NQ + p % NQ], p, p // (2 * NQ))
        with jax.named_scope("renorm_2"):
            each(4 * NQ, renorm_2)

        def third(k):
            tile = order3(k)
            for u in range(2):
                half_load(tile, u, u).wait()
            full(2, tile, C.at[tile])

            @pl.when(k + 1 < 4 * NQ)
            def _():
                for u in range(2):
                    half_load(order3(k + 1), u, u).start()

            @pl.when(tile // NQ == z)
            def _():
                c_local(tile).start()

            @pl.when(tile // NQ != z)
            def _():
                c_remote(tile).start()
        with jax.named_scope("third"):
            each(4 * NQ, third)

        def send_sums(k):
            @pl.when(k == me16)
            def _():
                home_sum_local().start()

            @pl.when(k != me16)
            def _():
                home_sum(k).start()
        each(16, send_sums)

    with jax.named_scope("home_wait"):
        done(chome, crecv)
    done(shome, hrecv)
    done(gfull.at[pl.ds(0, 2 * NQ), pl.ds(0, nb), :], zs)

    @pl.when(jnp.logical_not(is_mid))
    def _():
        done(abuf, asend)
        done(gfull.at[pl.ds(0, NQ), pl.ds(0, nb), :], ys)

    @pl.when(is_mid)
    def _():
        done(abuf.at[:, pl.ds(0, half), :], asend)
        done(gfull.at[pl.ds(0, 3 * NQ), pl.ds(0, nb), :], ys)
        done(gfull.at[pl.ds(0, 2 * NQ)], ps)
        done(C.at[pl.ds(0, 3 * NQ)], csend)

        def drain(k):
            @pl.when(k != me16)
            def _():
                home_sum(k).wait_send()
        each(16, drain)


def solution(mesh):
    block_spec = P(("graph", "row"), "col")

    def device_step(init_blk, graph_blk):
        nb = init_blk.shape[1]
        n, tw = 4 * nb, nb // NQ
        mb = min(512, nb // 2)
        dma = pltpu.SemaphoreType.DMA
        any_spec = pl.BlockSpec(memory_space=pl.ANY)
        m_home, s_home, _, _, _ = pl.pallas_call(
            functools.partial(mcl_kernel, nb, mb),
            out_shape=(
                jax.ShapeDtypeStruct((nb, nb), F32),
                jax.ShapeDtypeStruct((8, 1, nb), F32),
                jax.ShapeDtypeStruct((4 * NQ, n, tw), BF16),
                jax.ShapeDtypeStruct((NQ, nb, tw), BF16),
                jax.ShapeDtypeStruct((2 * NQ, nb // 2, tw), F32),
            ),
            in_specs=[any_spec] * 2,
            out_specs=[any_spec] * 5,
            scratch_shapes=[
                pltpu.VMEM((3, nb // 2, 2 * nb), BF16),
                pltpu.VMEM((4 * NQ, nb // 2, tw), F32),
                pltpu.VMEM((2, 2 * nb, tw), BF16),
                pltpu.VMEM((2, nb // 2, tw), F32),
                pltpu.VMEM((3, 8, 1, n), F32),
                pltpu.VMEM((1, n), F32),
                dma((2 * NQ,)),
                dma(()),
                dma((2,)),
                dma((2,)),
                dma(()),
                dma(()),
                dma((2, 4 * NQ, NS)),
                dma((4 * NQ,)),
                dma(()),
                dma(()),
                dma(()),
                dma((3,)),
                dma((3,)),
                dma(()),
                dma(()),
                dma(()),
                dma((16,)),
            ],
            compiler_params=pltpu.CompilerParams(
                collective_id=0, has_side_effects=True, vmem_limit_bytes=67043328),
            name="mcl",
        )(init_blk, graph_blk)
        col_sum = jnp.sum(s_home, axis=(0, 1))
        return m_home * (n / col_sum)

    return jax.shard_map(device_step, mesh=mesh, in_specs=(block_spec, block_spec), out_specs=block_spec, check_vma=False)
```

```python
import functools

import jax
import jax.numpy as jnp
from jax import lax
from jax.experimental import pallas as pl
from jax.experimental.pallas import tpu as pltpu
from jax.sharding import PartitionSpec as P

ITERATIONS = 3
NQ = 8
NS = 2
MESH = pl.DeviceIdType.MESH
F32, BF16 = jnp.float32, jnp.bfloat16


def mcl_kernel(nb, mb, a_hbm, g_hbm, chome, shome, gfull, abuf, m1b, AA, C, gt, st, Sx, scale,
               ld_sem, put_sem, tl_sem, st_sem, m1_sem, arecv, asend, grecv, precv, zs, ys, ps, sr, ss, crecv, csend, hrecv, hsend):
    tw = nb // NQ
    half = nb // 2
    sub = nb // NS
    order_n = 4 * nb
    z, i = lax.axis_index("col"), lax.axis_index("row")
    y, c = i // 2, i % 2
    side = z // 2
    mid, omid, end, oend = 1 + side, 2 - side, 3 * side, 3 - 3 * side
    is_mid = z == mid
    iy, ip = (1 - y) * 2 + c, y * 2 + (1 - c)
    iyp = (1 - y) * 2 + (1 - c)

    def pos(zz):
        return jnp.where(zz == 0, 2, jnp.where(zz == 3, 3, zz - 1))

    def spos(tile):
        return pos(tile // NQ) * NQ + tile % NQ

    def cols(q):
        return pl.ds(pl.multiple_of(q * tw, tw), tw)

    def halfrows(h):
        return pl.ds(pl.multiple_of(h * half, half), half)

    def gref(ii, tile, s):
        return gfull.at[tile, pl.ds(pl.multiple_of(pos(ii) * nb + s * sub, sub), sub), :]

    def gcopy(ii, tile, s, ssem, rsem, col, row):
        return pltpu.make_async_remote_copy(
            src_ref=gref(ii, tile, s), dst_ref=gref(ii, tile, s), send_sem=ssem, recv_sem=rsem,
            device_id={"col": col, "row": row}, device_id_type=MESH)

    def zcopy(ii, tile, s, col):
        return gcopy(ii, tile, s, zs, grecv.at[ii // 2, tile, s], col, i)

    def ycopy(tile, s):
        return gcopy(i, tile, s, ys, grecv.at[i // 2, tile, s], z, iy)

    def pcopy(ii, tile, s):
        return gcopy(ii, tile, s, ps, precv.at[tile], z, ip)

    def done(ref, sem):
        pltpu.make_async_copy(ref, ref, sem).wait()

    def gwait(ii, tile, s):
        done(gref(ii, tile, s), grecv.at[ii // 2, tile, s])

    def loads(src, base, q, h):
        return pltpu.make_async_copy(src.at[halfrows(h), cols(q)], C.at[base + 2 * q + h], ld_sem.at[base // 2 + q])

    def each(n, body):
        def step(k, carry):
            body(k)
            return carry
        lax.fori_loop(0, n, step, 0)

    def start_loads(q):
        for h in range(2):
            loads(a_hbm, 0, q, h).start()
            loads(g_hbm, 2 * NQ, q, h).start()
    each(NQ, start_loads)

    barrier = pltpu.get_barrier_semaphore()
    me16 = z * 4 + i

    def knock(d):
        other = lax.rem(me16 + 1 + d, 16)
        pl.semaphore_signal(barrier, inc=1, device_id={"col": other // 4, "row": other % 4}, device_id_type=MESH)
    each(15, knock)
    pl.semaphore_wait(barrier, 15)

    def a_dst(zz, q):
        return AA.at[pos(zz) // 2, :, cols(pos(zz) % 2 * NQ + q)]

    def a_remote(q, h):
        return pltpu.make_async_remote_copy(
            src_ref=abuf.at[q, halfrows(h), :], dst_ref=a_dst(z, q),
            send_sem=asend, recv_sem=arecv, device_id={"col": 1 + h, "row": i}, device_id_type=MESH)

    def a_local(q, h):
        return pltpu.make_async_copy(abuf.at[q, halfrows(h), :], a_dst(z, q), arecv)

    def cast(src, base, q, dst):
        done(C.at[pl.ds(base + 2 * q, 2)], ld_sem.at[base // 2 + q])
        for h in range(2):
            gt[0, h * half:(h + 1) * half, :] = C[base + 2 * q + h].astype(BF16)
        put = pltpu.make_async_copy(gt.at[0, pl.ds(0, nb), :], dst, put_sem)
        put.start()
        put.wait()

    def hand_out(q):
        cast(a_hbm, 0, q, abuf.at[q])
        for h in range(2):
            @pl.when(z == 1 + h)
            def _():
                a_local(q, h).start()

            @pl.when(z != 1 + h)
            def _():
                a_remote(q, h).start()
        tile = z * NQ + q
        cast(g_hbm, 2 * NQ, q, gfull.at[tile, pl.ds(pl.multiple_of(pos(i) * nb, nb), nb), :])
        for s in range(NS):
            ycopy(tile, s).start()

            @pl.when(is_mid)
            def _():
                pcopy(i, tile, s).start()
    with jax.named_scope("hand_out"):
        each(NQ, hand_out)

    @pl.when(jnp.logical_not(is_mid))
    def _():
        def relay(q):
            tile = z * NQ + q
            for s in range(NS):
                zcopy(i, tile, s, mid).start()
            for s in range(NS):
                gwait(iy, tile, s)
                zcopy(iy, tile, s, mid).start()
        each(NQ, relay)

    def mtile(t):
        return jnp.where(t < NQ, omid * NQ + t, oend * NQ + t - NQ)

    def own_z(q):
        for s in range(NS):
            zcopy(i, z * NQ + q, s, omid).start()

    def y_pass(t):
        tm = mtile(t)
        for s in range(NS):
            gwait(iy, tm, s)
            pcopy(iy, tm, s).start()

    def z_pass(t):
        tm = mtile(t)
        for s in range(NS):
            gwait(i, tm, s)
            ycopy(tm, s).start()
            pcopy(i, tm, s).start()

        @pl.when(t < NQ - 2)
        def _():
            own_z(t + 2)
        te = end * NQ + t // 2
        odd = t % 2

        @pl.when(odd == 0)
        def _():
            for s in range(NS):
                gwait(i, te, s)
                pcopy(i, te, s).start()

        @pl.when(odd == 1)
        def _():
            for s in range(NS):
                gwait(iy, te, s)
                pcopy(iy, te, s).start()

        @pl.when(jnp.logical_or(jnp.logical_and(t >= NQ - 2, t <= 2 * NQ - 4), t == 2 * NQ - 2))
        def _():
            for s in range(NS):
                zcopy(i, end * NQ + jnp.minimum(t - NQ + 2, NQ - 1), s, omid).start()

    me8 = (z - 1) * 4 + i

    def half_load(tile, k, slot):
        return pltpu.make_async_copy(
            gfull.at[tile, pl.ds(pl.multiple_of(k * 2 * nb, 2 * nb), 2 * nb), :], gt.at[slot], tl_sem.at[slot])

    def blocks(body):
        def step(m, s):
            return body(pl.ds(pl.multiple_of(m * mb, mb), mb), s)
        return lax.fori_loop(0, half // mb, step, jnp.zeros((8, tw), F32))

    def fold(sq):
        return jnp.sum(sq.reshape(mb // 8, 8, tw), axis=0)

    def put_sum(it, tile, s):
        Sx[it, me8, :, cols(spos(tile))] = jnp.sum(s, axis=0, keepdims=True)

    def full(it, tile, dst):
        def block(r, s):
            acc = jnp.dot(AA[0, r, :], gt[0], preferred_element_type=F32)
            acc = acc + jnp.dot(AA[1, r, :], gt[1], preferred_element_type=F32)
            sq = acc * acc
            dst[r, :] = sq
            return s + fold(sq)
        put_sum(it, tile, blocks(block))

    def first_half(tile, slot):
        def block(r, s):
            C[tile, r, :] = jnp.dot(AA[2, r, :], gt[slot], preferred_element_type=F32)
            return s
        blocks(block)

    def second_half(tile, slot):
        def block(r, s):
            acc = C[tile, r, :] + jnp.dot(AA[1, r, :], gt[slot], preferred_element_type=F32)
            sq = acc * acc
            C[tile, r, :] = sq
            return s + fold(sq)
        put_sum(1, tile, blocks(block))

    def s_ref(part, src, n):
        if part < 2:
            return Sx.at[0, pl.ds(src, n), :, pl.ds(part * 2 * nb, 2 * nb)]
        return Sx.at[1, pl.ds(src, n)]

    def s_start(part):
        def send(d):
            other = lax.rem(me8 + d + 1, 8)
            pltpu.make_async_remote_copy(
                src_ref=s_ref(part, me8, 1), dst_ref=s_ref(part, me8, 1), send_sem=ss.at[part], recv_sem=sr.at[part],
                device_id={"col": 1 + other // 4, "row": other % 4}, device_id_type=MESH).start()
        each(7, send)

    def s_finish(part):
        done(s_ref(part, 0, 7), sr.at[part])
        lo, n, it = (part * 2 * nb, 2 * nb, 0) if part < 2 else (0, 4 * nb, 1)
        total = Sx[it, 0, :, lo:lo + n]
        for k in range(1, 8):
            total = total + Sx[it, k, :, lo:lo + n]
        scale[:, lo:lo + n] = float(order_n) / total
        done(s_ref(part, 0, 7), ss.at[part])

    def renorm(src, p, buf):
        fac = scale[:, cols(p)]

        def part(m):
            r = pl.ds(pl.multiple_of(m * mb, mb), mb)
            AA[buf, r, cols(p % (2 * NQ))] = (src[r, :] * fac).astype(BF16)
        each(half // mb, part)

    def b_number(tile):
        return jnp.where(tile // NQ == end, tile % NQ, NQ + tile % NQ)

    def m1_put(tile):
        k = b_number(tile)
        return pltpu.make_async_copy(C.at[tile], m1b.at[k], m1_sem.at[k])

    def m1_get(slot, k):
        return pltpu.make_async_copy(m1b.at[k], st.at[slot], st_sem.at[slot])

    def order3(k):
        j = k - NQ
        both = jnp.where(j % 2 == 0, omid, end) * NQ + j // 2
        return jnp.where(k < NQ, oend * NQ + k, jnp.where(k < 3 * NQ, both, mid * NQ + k - 3 * NQ))

    def c_remote(tile):
        q = tile % NQ
        return pltpu.make_async_remote_copy(
            src_ref=C.at[tile], dst_ref=chome.at[halfrows(z - 1), cols(q)],
            send_sem=csend, recv_sem=crecv,
            device_id={"col": tile // NQ, "row": i}, device_id_type=MESH)

    def c_local(tile):
        q = tile % NQ
        return pltpu.make_async_copy(C.at[tile], chome.at[halfrows(z - 1), cols(q)], crecv)

    def home_sum(k):
        zz, ii = k // 4, k % 4
        return pltpu.make_async_remote_copy(
            src_ref=Sx.at[2, me8, :, pl.ds(pl.multiple_of(pos(zz) * nb, nb), nb)], dst_ref=shome.at[me8],
            send_sem=hsend.at[k], recv_sem=hrecv,
            device_id={"col": zz, "row": ii}, device_id_type=MESH)

    def home_sum_local():
        return pltpu.make_async_copy(
            Sx.at[2, me8, :, pl.ds(pl.multiple_of(pos(z) * nb, nb), nb)], shome.at[me8], hrecv)

    @pl.when(is_mid)
    def _():
        own_z(0)
        own_z(1)

        def own_y(q):
            tile = z * NQ + q
            for s in range(NS):
                gwait(iy, tile, s)
                pcopy(iy, tile, s).start()
        with jax.named_scope("own_y"):
            each(NQ, own_y)

        with jax.named_scope("a_wait"):
            done(AA.at[pl.ds(0, 2)], arecv)

        def fetch(tile):
            done(gfull.at[tile, pl.ds(0, 2 * nb), :], precv.at[tile])
            for k in range(2):
                half_load(tile, k, k).start()
            for k in range(2):
                half_load(tile, k, k).wait()

        def own_cols(k):
            @pl.when(k == NQ // 2)
            def _():
                z_pass(0)
            tile = mid * NQ + k
            fetch(tile)
            full(0, tile, C.at[tile])
        with jax.named_scope("own_cols"):
            each(NQ, own_cols)

        def extra(e):
            f = e - 2 * NQ - 6
            late = jnp.where(f % 3 == 2, end * NQ + 5 + f // 3, oend * NQ + 1 + 2 * (f // 3) + f % 3)
            b = jnp.where(e < 2 * NQ + 5, end * NQ + e - 2 * NQ, oend * NQ)
            return jnp.where(e < 2 * NQ, NQ + e, jnp.where(f < 0, b, late))

        def extra_range(t):
            odd = t % 2
            lo = jnp.where(t < 10, 0, 4 + 9 * ((t - 10) // 2) + 6 * odd)
            n = jnp.where(t < 10, 4, jnp.where(t == 2 * NQ, 1, 6 - 3 * odd))
            return lo, n

        def slot_step(k):
            t = k + 1
            odd = t % 2
            lo, n = extra_range(t)
            with jax.named_scope("y_pass"):
                y_pass(t - 1)
            tile = mtile(t - 1)
            with jax.named_scope("fetch_m"):
                fetch(tile)
            full(0, tile, C.at[tile])

            @pl.when(t > NQ)
            def _():
                m1_put(tile).start()

            @pl.when(t == NQ)
            def _():
                s_start(0)
            early = jnp.logical_and(t > NQ, odd == 0)

            @pl.when(early)
            def _():
                half_load(extra(lo), 0, 0).start()

            @pl.when(t < 2 * NQ)
            def _():
                with jax.named_scope("z_pass"):
                    z_pass(t)

            @pl.when(odd == 1)
            def _():
                te = end * NQ + t // 2
                with jax.named_scope("fetch_e"):
                    fetch(te)
                full(0, te, C.at[te])
                m1_put(te).start()

            @pl.when(t == NQ + 1)
            def _():
                with jax.named_scope("sums0"):
                    s_finish(0)

                def renorm_a(p):
                    zz = 1 + p // NQ
                    renorm(C.at[zz * NQ + p % NQ], p, 2)
                each(2 * NQ, renorm_a)

            @pl.when(t > NQ)
            def _():
                @pl.when(odd == 1)
                def _():
                    half_load(extra(lo), 0, 0).start()

                def part(u, carry):
                    slot = u % 2
                    te = extra(lo + u)

                    @pl.when(u + 1 < n)
                    def _():
                        half_load(extra(lo + u + 1), 0, 1 - slot).start()
                    half_load(0, 0, slot).wait()

                    @pl.when(lo + u >= 2 * NQ)
                    def _():
                        m1_put(te).wait()
                    first_half(te, slot)
                    return carry
                with jax.named_scope("extra"):
                    lax.fori_loop(0, n, part, 0)
        each(2 * NQ, slot_step)
        half_load(0, 1, 0).start()
        half_load(NQ, 1, 1).start()
        def b_index(p):
            zz = jnp.where(p < NQ, 0, 3)
            return b_number(zz * NQ + p % NQ)

        for slot in range(2):
            m1_get(slot, b_index(slot)).start()
        s_start(1)
        with jax.named_scope("sums1"):
            s_finish(1)

        def renorm_b(p):
            slot = p % 2
            m1_get(slot, 0).wait()
            renorm(st.at[slot], 2 * NQ + p, 1)

            @pl.when(p + 2 < 2 * NQ)
            def _():
                m1_get(slot, b_index(p + 2)).start()
        with jax.named_scope("renorm_b"):
            each(2 * NQ, renorm_b)

        def order2(k):
            return (k % 4) * NQ + k // 4

        def second(k):
            slot = k % 2
            tile = order2(k)
            half_load(tile, 1, slot).wait()
            second_half(tile, slot)

            @pl.when(k + 2 < 4 * NQ)
            def _():
                half_load(order2(k + 2), 1, slot).start()
        with jax.named_scope("second"):
            each(4 * NQ, second)
        for k in range(2):
            half_load(order3(0), k, k).start()
        s_start(2)
        with jax.named_scope("sums2"):
            s_finish(2)

        def renorm_2(p):
            pz = p // NQ
            zz = jnp.where(pz == 2, 0, jnp.where(pz == 3, 3, pz + 1))
            renorm(C.at[zz * NQ + p % NQ], p, p // (2 * NQ))
        with jax.named_scope("renorm_2"):
            each(4 * NQ, renorm_2)

        def third(k):
            tile = order3(k)
            for u in range(2):
                half_load(tile, u, u).wait()
            full(2, tile, C.at[tile])

            @pl.when(k + 1 < 4 * NQ)
            def _():
                for u in range(2):
                    half_load(order3(k + 1), u, u).start()

            @pl.when(tile // NQ == z)
            def _():
                c_local(tile).start()

            @pl.when(tile // NQ != z)
            def _():
                c_remote(tile).start()
        with jax.named_scope("third"):
            each(4 * NQ, third)

        def send_sums(k):
            @pl.when(k == me16)
            def _():
                home_sum_local().start()

            @pl.when(k != me16)
            def _():
                home_sum(k).start()
        each(16, send_sums)

    with jax.named_scope("home_wait"):
        done(chome, crecv)
    done(shome, hrecv)
    done(gfull.at[pl.ds(0, 2 * NQ), pl.ds(0, nb), :], zs)

    @pl.when(jnp.logical_not(is_mid))
    def _():
        done(abuf, asend)
        done(gfull.at[pl.ds(0, NQ), pl.ds(0, nb), :], ys)

    @pl.when(is_mid)
    def _():
        done(abuf.at[:, pl.ds(0, half), :], asend)
        done(gfull.at[pl.ds(0, 3 * NQ), pl.ds(0, nb), :], ys)
        done(gfull.at[pl.ds(0, 2 * NQ)], ps)
        done(C.at[pl.ds(0, 3 * NQ)], csend)

        def drain(k):
            @pl.when(k != me16)
            def _():
                home_sum(k).wait_send()
        each(16, drain)


def solution(mesh):
    block_spec = P(("graph", "row"), "col")

    def device_step(init_blk, graph_blk):
        nb = init_blk.shape[1]
        n, tw = 4 * nb, nb // NQ
        mb = min(512, nb // 2)
        dma = pltpu.SemaphoreType.DMA
        any_spec = pl.BlockSpec(memory_space=pl.ANY)
        m_home, s_home, _, _, _ = pl.pallas_call(
            functools.partial(mcl_kernel, nb, mb),
            out_shape=(
                jax.ShapeDtypeStruct((nb, nb), F32),
                jax.ShapeDtypeStruct((8, 1, nb), F32),
                jax.ShapeDtypeStruct((4 * NQ, n, tw), BF16),
                jax.ShapeDtypeStruct((NQ, nb, tw), BF16),
                jax.ShapeDtypeStruct((2 * NQ, nb // 2, tw), F32),
            ),
            in_specs=[any_spec] * 2,
            out_specs=[any_spec] * 5,
            scratch_shapes=[
                pltpu.VMEM((3, nb // 2, 2 * nb), BF16),
                pltpu.VMEM((4 * NQ, nb // 2, tw), F32),
                pltpu.VMEM((2, 2 * nb, tw), BF16),
                pltpu.VMEM((2, nb // 2, tw), F32),
                pltpu.VMEM((3, 8, 1, n), F32),
                pltpu.VMEM((1, n), F32),
                dma((2 * NQ,)),
                dma(()),
                dma((2,)),
                dma((2,)),
                dma((2 * NQ,)),
                dma(()),
                dma(()),
                dma((2, 4 * NQ, NS)),
                dma((4 * NQ,)),
                dma(()),
                dma(()),
                dma(()),
                dma((3,)),
                dma((3,)),
                dma(()),
                dma(()),
                dma(()),
                dma((16,)),
            ],
            compiler_params=pltpu.CompilerParams(
                collective_id=0, has_side_effects=True, vmem_limit_bytes=67043328),
            name="mcl",
        )(init_blk, graph_blk)
        col_sum = jnp.sum(s_home, axis=(0, 1))
        return m_home * (n / col_sum)

    return jax.shard_map(device_step, mesh=mesh, in_specs=(block_spec, block_spec), out_specs=block_spec, check_vma=False)
```

```python
import functools

import jax
import jax.numpy as jnp
from jax import lax
from jax.experimental import pallas as pl
from jax.experimental.pallas import tpu as pltpu
from jax.sharding import PartitionSpec as P

ITERATIONS = 3
NQ = 8
NS = 2
MESH = pl.DeviceIdType.MESH
F32, BF16 = jnp.float32, jnp.bfloat16


def mcl_kernel(nb, mb, a_hbm, g_hbm, chome, shome, gfull, abuf, m1b, AA, C, gt, st, Sx, scale,
               ld_sem, put_sem, tl_sem, st_sem, m1_sem, arecv, asend, grecv, precv, zs, ys, ps, sr, ss, crecv, csend, hrecv, hsend):
    tw = nb // NQ
    half = nb // 2
    sub = nb // NS
    order_n = 4 * nb
    z, i = lax.axis_index("col"), lax.axis_index("row")
    y, c = i // 2, i % 2
    side = z // 2
    mid, omid, end, oend = 1 + side, 2 - side, 3 * side, 3 - 3 * side
    is_mid = z == mid
    iy, ip = (1 - y) * 2 + c, y * 2 + (1 - c)
    iyp = (1 - y) * 2 + (1 - c)

    def pos(zz):
        return jnp.where(zz == 0, 2, jnp.where(zz == 3, 3, zz - 1))

    def spos(tile):
        return pos(tile // NQ) * NQ + tile % NQ

    def cols(q):
        return pl.ds(pl.multiple_of(q * tw, tw), tw)

    def halfrows(h):
        return pl.ds(pl.multiple_of(h * half, half), half)

    def gref(ii, tile, s):
        return gfull.at[tile, pl.ds(pl.multiple_of(pos(ii) * nb + s * sub, sub), sub), :]

    def gcopy(ii, tile, s, ssem, rsem, col, row):
        return pltpu.make_async_remote_copy(
            src_ref=gref(ii, tile, s), dst_ref=gref(ii, tile, s), send_sem=ssem, recv_sem=rsem,
            device_id={"col": col, "row": row}, device_id_type=MESH)

    def zcopy(ii, tile, s, col):
        return gcopy(ii, tile, s, zs, grecv.at[ii // 2, tile, s], col, i)

    def ycopy(tile, s):
        return gcopy(i, tile, s, ys, grecv.at[i // 2, tile, s], z, iy)

    def pcopy(ii, tile, s):
        return gcopy(ii, tile, s, ps, precv.at[tile], z, ip)

    def done(ref, sem):
        pltpu.make_async_copy(ref, ref, sem).wait()

    def gwait(ii, tile, s):
        done(gref(ii, tile, s), grecv.at[ii // 2, tile, s])

    def loads(src, base, q, h):
        return pltpu.make_async_copy(src.at[halfrows(h), cols(q)], C.at[base + 2 * q + h], ld_sem.at[base // 2 + q])

    def each(n, body):
        def step(k, carry):
            body(k)
            return carry
        lax.fori_loop(0, n, step, 0)

    def start_loads(q):
        for h in range(2):
            loads(a_hbm, 0, q, h).start()
            loads(g_hbm, 2 * NQ, q, h).start()
    each(NQ, start_loads)

    barrier = pltpu.get_barrier_semaphore()
    me16 = z * 4 + i

    def knock(d):
        other = lax.rem(me16 + 1 + d, 16)
        pl.semaphore_signal(barrier, inc=1, device_id={"col": other // 4, "row": other % 4}, device_id_type=MESH)
    each(15, knock)
    pl.semaphore_wait(barrier, 15)

    def a_dst(zz, q):
        return AA.at[pos(zz) // 2, :, cols(pos(zz) % 2 * NQ + q)]

    def a_remote(q, h):
        return pltpu.make_async_remote_copy(
            src_ref=abuf.at[q, halfrows(h), :], dst_ref=a_dst(z, q),
            send_sem=asend, recv_sem=arecv, device_id={"col": 1 + h, "row": i}, device_id_type=MESH)

    def a_local(q, h):
        return pltpu.make_async_copy(abuf.at[q, halfrows(h), :], a_dst(z, q), arecv)

    def cast(src, base, q, dst):
        done(C.at[pl.ds(base + 2 * q, 2)], ld_sem.at[base // 2 + q])
        for h in range(2):
            gt[0, h * half:(h + 1) * half, :] = C[base + 2 * q + h].astype(BF16)
        put = pltpu.make_async_copy(gt.at[0, pl.ds(0, nb), :], dst, put_sem)
        put.start()
        put.wait()

    def hand_out(q):
        cast(a_hbm, 0, q, abuf.at[q])
        for h in range(2):
            @pl.when(z == 1 + h)
            def _():
                a_local(q, h).start()

            @pl.when(z != 1 + h)
            def _():
                a_remote(q, h).start()
        tile = z * NQ + q
        cast(g_hbm, 2 * NQ, q, gfull.at[tile, pl.ds(pl.multiple_of(pos(i) * nb, nb), nb), :])
        for s in range(NS):
            ycopy(tile, s).start()

            @pl.when(is_mid)
            def _():
                pcopy(i, tile, s).start()
    with jax.named_scope("hand_out"):
        each(NQ, hand_out)

    @pl.when(jnp.logical_not(is_mid))
    def _():
        def relay(q):
            tile = z * NQ + q
            for s in range(NS):
                zcopy(i, tile, s, mid).start()
            for s in range(NS):
                gwait(iy, tile, s)
                zcopy(iy, tile, s, mid).start()
        each(NQ, relay)

    def mtile(t):
        return jnp.where(t < NQ, omid * NQ + t, oend * NQ + t - NQ)

    def own_z(q):
        for s in range(NS):
            zcopy(i, z * NQ + q, s, omid).start()

    def y_pass(t):
        tm = mtile(t)
        for s in range(NS):
            gwait(iy, tm, s)
            pcopy(iy, tm, s).start()

    def z_pass(t):
        tm = mtile(t)
        for s in range(NS):
            gwait(i, tm, s)
            ycopy(tm, s).start()
            pcopy(i, tm, s).start()
        te = end * NQ + t // 2
        odd = t % 2

        @pl.when(odd == 0)
        def _():
            for s in range(NS):
                gwait(i, te, s)
                pcopy(i, te, s).start()

        @pl.when(odd == 1)
        def _():
            for s in range(NS):
                gwait(iy, te, s)
                pcopy(iy, te, s).start()

    def z_issue(t):
        @pl.when(t < NQ - 2)
        def _():
            own_z(t + 2)

        @pl.when(jnp.logical_or(jnp.logical_and(t >= NQ - 2, t <= 2 * NQ - 4), t == 2 * NQ - 2))
        def _():
            for s in range(NS):
                zcopy(i, end * NQ + jnp.minimum(t - NQ + 2, NQ - 1), s, omid).start()

    me8 = (z - 1) * 4 + i

    def half_load(tile, k, slot):
        return pltpu.make_async_copy(
            gfull.at[tile, pl.ds(pl.multiple_of(k * 2 * nb, 2 * nb), 2 * nb), :], gt.at[slot], tl_sem.at[slot])

    def blocks(body):
        def step(m, s):
            return body(pl.ds(pl.multiple_of(m * mb, mb), mb), s)
        return lax.fori_loop(0, half // mb, step, jnp.zeros((8, tw), F32))

    def fold(sq):
        return jnp.sum(sq.reshape(mb // 8, 8, tw), axis=0)

    def put_sum(it, tile, s):
        Sx[it, me8, :, cols(spos(tile))] = jnp.sum(s, axis=0, keepdims=True)

    def full(it, tile, dst):
        def block(r, s):
            acc = jnp.dot(AA[0, r, :], gt[0], preferred_element_type=F32)
            acc = acc + jnp.dot(AA[1, r, :], gt[1], preferred_element_type=F32)
            sq = acc * acc
            dst[r, :] = sq
            return s + fold(sq)
        put_sum(it, tile, blocks(block))

    def first_half(tile, slot):
        def block(r, s):
            C[tile, r, :] = jnp.dot(AA[2, r, :], gt[slot], preferred_element_type=F32)
            return s
        blocks(block)

    def second_half(tile, slot):
        def block(r, s):
            acc = C[tile, r, :] + jnp.dot(AA[1, r, :], gt[slot], preferred_element_type=F32)
            sq = acc * acc
            C[tile, r, :] = sq
            return s + fold(sq)
        put_sum(1, tile, blocks(block))

    def s_ref(part, src, n):
        if part < 2:
            return Sx.at[0, pl.ds(src, n), :, pl.ds(part * 2 * nb, 2 * nb)]
        return Sx.at[1, pl.ds(src, n)]

    def s_start(part):
        def send(d):
            other = lax.rem(me8 + d + 1, 8)
            pltpu.make_async_remote_copy(
                src_ref=s_ref(part, me8, 1), dst_ref=s_ref(part, me8, 1), send_sem=ss.at[part], recv_sem=sr.at[part],
                device_id={"col": 1 + other // 4, "row": other % 4}, device_id_type=MESH).start()
        each(7, send)

    def s_finish(part):
        done(s_ref(part, 0, 7), sr.at[part])
        lo, n, it = (part * 2 * nb, 2 * nb, 0) if part < 2 else (0, 4 * nb, 1)
        total = Sx[it, 0, :, lo:lo + n]
        for k in range(1, 8):
            total = total + Sx[it, k, :, lo:lo + n]
        scale[:, lo:lo + n] = float(order_n) / total
        done(s_ref(part, 0, 7), ss.at[part])

    def renorm(src, p, buf):
        fac = scale[:, cols(p)]

        def part(m):
            r = pl.ds(pl.multiple_of(m * mb, mb), mb)
            AA[buf, r, cols(p % (2 * NQ))] = (src[r, :] * fac).astype(BF16)
        each(half // mb, part)

    def b_number(tile):
        return jnp.where(tile // NQ == end, tile % NQ, NQ + tile % NQ)

    def m1_put(tile):
        k = b_number(tile)
        return pltpu.make_async_copy(C.at[tile], m1b.at[k], m1_sem.at[k])

    def m1_get(slot, k):
        return pltpu.make_async_copy(m1b.at[k], st.at[slot], st_sem.at[slot])

    def order3(k):
        j = k - NQ
        both = jnp.where(j % 2 == 0, omid, end) * NQ + j // 2
        return jnp.where(k < NQ, oend * NQ + k, jnp.where(k < 3 * NQ, both, mid * NQ + k - 3 * NQ))

    def c_remote(tile):
        q = tile % NQ
        return pltpu.make_async_remote_copy(
            src_ref=C.at[tile], dst_ref=chome.at[halfrows(z - 1), cols(q)],
            send_sem=csend, recv_sem=crecv,
            device_id={"col": tile // NQ, "row": i}, device_id_type=MESH)

    def c_local(tile):
        q = tile % NQ
        return pltpu.make_async_copy(C.at[tile], chome.at[halfrows(z - 1), cols(q)], crecv)

    def home_sum(k):
        zz, ii = k // 4, k % 4
        return pltpu.make_async_remote_copy(
            src_ref=Sx.at[2, me8, :, pl.ds(pl.multiple_of(pos(zz) * nb, nb), nb)], dst_ref=shome.at[me8],
            send_sem=hsend.at[k], recv_sem=hrecv,
            device_id={"col": zz, "row": ii}, device_id_type=MESH)

    def home_sum_local():
        return pltpu.make_async_copy(
            Sx.at[2, me8, :, pl.ds(pl.multiple_of(pos(z) * nb, nb), nb)], shome.at[me8], hrecv)

    @pl.when(is_mid)
    def _():
        own_z(0)
        own_z(1)

        def own_y(q):
            tile = z * NQ + q
            for s in range(NS):
                gwait(iy, tile, s)
                pcopy(iy, tile, s).start()
        with jax.named_scope("own_y"):
            each(NQ, own_y)

        with jax.named_scope("a_wait"):
            done(AA.at[pl.ds(0, 2)], arecv)

        def fetch(tile):
            done(gfull.at[tile, pl.ds(0, 2 * nb), :], precv.at[tile])
            for k in range(2):
                half_load(tile, k, k).start()
            for k in range(2):
                half_load(tile, k, k).wait()

        def own_cols(k):
            @pl.when(k == NQ // 2)
            def _():
                z_pass(0)
                z_issue(0)
            tile = mid * NQ + k
            fetch(tile)
            full(0, tile, C.at[tile])
        with jax.named_scope("own_cols"):
            each(NQ, own_cols)

        def extra(e):
            f = e - 2 * NQ - 6
            late = jnp.where(f % 3 == 2, end * NQ + 5 + f // 3, oend * NQ + 1 + 2 * (f // 3) + f % 3)
            b = jnp.where(e < 2 * NQ + 5, end * NQ + e - 2 * NQ, oend * NQ)
            return jnp.where(e < 2 * NQ, NQ + e, jnp.where(f < 0, b, late))

        def extra_range(t):
            odd = t % 2
            lo = jnp.where(t < 10, 0, 4 + 9 * ((t - 10) // 2) + 6 * odd)
            n = jnp.where(t < 10, 4, jnp.where(t == 2 * NQ, 1, 6 - 3 * odd))
            return lo, n

        def slot_step(k):
            t = k + 1
            odd = t % 2
            lo, n = extra_range(t)

            @pl.when(t < 2 * NQ)
            def _():
                with jax.named_scope("z_pass"):
                    z_pass(t)

                @pl.when(t != NQ)
                def _():
                    z_issue(t)
            with jax.named_scope("y_pass"):
                y_pass(t - 1)
            tile = mtile(t - 1)
            with jax.named_scope("fetch_m"):
                fetch(tile)
            full(0, tile, C.at[tile])

            @pl.when(t > NQ)
            def _():
                m1_put(tile).start()

            @pl.when(t == NQ)
            def _():
                s_start(0)
                z_issue(t)

            @pl.when(odd == 1)
            def _():
                te = end * NQ + t // 2
                with jax.named_scope("fetch_e"):
                    fetch(te)
                full(0, te, C.at[te])
                m1_put(te).start()

            @pl.when(t == NQ + 1)
            def _():
                with jax.named_scope("sums0"):
                    s_finish(0)

                def renorm_a(p):
                    zz = 1 + p // NQ
                    renorm(C.at[zz * NQ + p % NQ], p, 2)
                each(2 * NQ, renorm_a)

            @pl.when(t > NQ)
            def _():
                half_load(extra(lo), 0, 0).start()

                def part(u, carry):
                    slot = u % 2
                    te = extra(lo + u)

                    @pl.when(u + 1 < n)
                    def _():
                        half_load(extra(lo + u + 1), 0, 1 - slot).start()
                    half_load(0, 0, slot).wait()

                    @pl.when(lo + u >= 2 * NQ)
                    def _():
                        m1_put(te).wait()
                    first_half(te, slot)
                    return carry
                with jax.named_scope("extra"):
                    lax.fori_loop(0, n, part, 0)
        each(2 * NQ, slot_step)
        half_load(0, 1, 0).start()
        half_load(NQ, 1, 1).start()
        def b_index(p):
            zz = jnp.where(p < NQ, 0, 3)
            return b_number(zz * NQ + p % NQ)

        for slot in range(2):
            m1_get(slot, b_index(slot)).start()
        s_start(1)
        with jax.named_scope("sums1"):
            s_finish(1)

        def renorm_b(p):
            slot = p % 2
            m1_get(slot, 0).wait()
            renorm(st.at[slot], 2 * NQ + p, 1)

            @pl.when(p + 2 < 2 * NQ)
            def _():
                m1_get(slot, b_index(p + 2)).start()
        with jax.named_scope("renorm_b"):
            each(2 * NQ, renorm_b)

        def order2(k):
            return (k % 4) * NQ + k // 4

        def second(k):
            slot = k % 2
            tile = order2(k)
            half_load(tile, 1, slot).wait()
            second_half(tile, slot)

            @pl.when(k + 2 < 4 * NQ)
            def _():
                half_load(order2(k + 2), 1, slot).start()
        with jax.named_scope("second"):
            each(4 * NQ, second)
        for k in range(2):
            half_load(order3(0), k, k).start()
        s_start(2)
        with jax.named_scope("sums2"):
            s_finish(2)

        def renorm_2(p):
            pz = p // NQ
            zz = jnp.where(pz == 2, 0, jnp.where(pz == 3, 3, pz + 1))
            renorm(C.at[zz * NQ + p % NQ], p, p // (2 * NQ))
        with jax.named_scope("renorm_2"):
            each(4 * NQ, renorm_2)

        def third(k):
            tile = order3(k)
            for u in range(2):
                half_load(tile, u, u).wait()
            full(2, tile, C.at[tile])

            @pl.when(k + 1 < 4 * NQ)
            def _():
                for u in range(2):
                    half_load(order3(k + 1), u, u).start()

            @pl.when(tile // NQ == z)
            def _():
                c_local(tile).start()

            @pl.when(tile // NQ != z)
            def _():
                c_remote(tile).start()
        with jax.named_scope("third"):
            each(4 * NQ, third)

        def send_sums(k):
            @pl.when(k == me16)
            def _():
                home_sum_local().start()

            @pl.when(k != me16)
            def _():
                home_sum(k).start()
        each(16, send_sums)

    with jax.named_scope("home_wait"):
        done(chome, crecv)
    done(shome, hrecv)
    done(gfull.at[pl.ds(0, 2 * NQ), pl.ds(0, nb), :], zs)

    @pl.when(jnp.logical_not(is_mid))
    def _():
        done(abuf, asend)
        done(gfull.at[pl.ds(0, NQ), pl.ds(0, nb), :], ys)

    @pl.when(is_mid)
    def _():
        done(abuf.at[:, pl.ds(0, half), :], asend)
        done(gfull.at[pl.ds(0, 3 * NQ), pl.ds(0, nb), :], ys)
        done(gfull.at[pl.ds(0, 2 * NQ)], ps)
        done(C.at[pl.ds(0, 3 * NQ)], csend)

        def drain(k):
            @pl.when(k != me16)
            def _():
                home_sum(k).wait_send()
        each(16, drain)


def solution(mesh):
    block_spec = P(("graph", "row"), "col")

    def device_step(init_blk, graph_blk):
        nb = init_blk.shape[1]
        n, tw = 4 * nb, nb // NQ
        mb = min(512, nb // 2)
        dma = pltpu.SemaphoreType.DMA
        any_spec = pl.BlockSpec(memory_space=pl.ANY)
        m_home, s_home, _, _, _ = pl.pallas_call(
            functools.partial(mcl_kernel, nb, mb),
            out_shape=(
                jax.ShapeDtypeStruct((nb, nb), F32),
                jax.ShapeDtypeStruct((8, 1, nb), F32),
                jax.ShapeDtypeStruct((4 * NQ, n, tw), BF16),
                jax.ShapeDtypeStruct((NQ, nb, tw), BF16),
                jax.ShapeDtypeStruct((2 * NQ, nb // 2, tw), F32),
            ),
            in_specs=[any_spec] * 2,
            out_specs=[any_spec] * 5,
            scratch_shapes=[
                pltpu.VMEM((3, nb // 2, 2 * nb), BF16),
                pltpu.VMEM((4 * NQ, nb // 2, tw), F32),
                pltpu.VMEM((2, 2 * nb, tw), BF16),
                pltpu.VMEM((2, nb // 2, tw), F32),
                pltpu.VMEM((3, 8, 1, n), F32),
                pltpu.VMEM((1, n), F32),
                dma((2 * NQ,)),
                dma(()),
                dma((2,)),
                dma((2,)),
                dma((2 * NQ,)),
                dma(()),
                dma(()),
                dma((2, 4 * NQ, NS)),
                dma((4 * NQ,)),
                dma(()),
                dma(()),
                dma(()),
                dma((3,)),
                dma((3,)),
                dma(()),
                dma(()),
                dma(()),
                dma((16,)),
            ],
            compiler_params=pltpu.CompilerParams(
                collective_id=0, has_side_effects=True, vmem_limit_bytes=67043328),
            name="mcl",
        )(init_blk, graph_blk)
        col_sum = jnp.sum(s_home, axis=(0, 1))
        return m_home * (n / col_sum)

    return jax.shard_map(device_step, mesh=mesh, in_specs=(block_spec, block_spec), out_specs=block_spec, check_vma=False)
```

```python
import functools

import jax
import jax.numpy as jnp
from jax import lax
from jax.experimental import pallas as pl
from jax.experimental.pallas import tpu as pltpu
from jax.sharding import PartitionSpec as P

ITERATIONS = 3
NQ = 8
NS = 2
MESH = pl.DeviceIdType.MESH
F32, BF16 = jnp.float32, jnp.bfloat16


def mcl_kernel(nb, mb, a_hbm, g_hbm, chome, shome, gfull, abuf, m1b, AA, C, gt, st, Sx, scale,
               ld_sem, put_sem, tl_sem, st_sem, m1_sem, arecv, asend, grecv, precv, zs, ys, ps, sr, ss, crecv, csend, hrecv, hsend):
    tw = nb // NQ
    half = nb // 2
    sub = nb // NS
    order_n = 4 * nb
    z, i = lax.axis_index("col"), lax.axis_index("row")
    y, c = i // 2, i % 2
    side = z // 2
    mid, omid, end, oend = 1 + side, 2 - side, 3 * side, 3 - 3 * side
    is_mid = z == mid
    iy, ip = (1 - y) * 2 + c, y * 2 + (1 - c)
    iyp = (1 - y) * 2 + (1 - c)

    def pos(zz):
        return jnp.where(zz == 0, 2, jnp.where(zz == 3, 3, zz - 1))

    def spos(tile):
        return pos(tile // NQ) * NQ + tile % NQ

    def cols(q):
        return pl.ds(pl.multiple_of(q * tw, tw), tw)

    def halfrows(h):
        return pl.ds(pl.multiple_of(h * half, half), half)

    def gref(ii, tile, s):
        return gfull.at[tile, pl.ds(pl.multiple_of(pos(ii) * nb + s * sub, sub), sub), :]

    def gcopy(ii, tile, s, ssem, rsem, col, row):
        return pltpu.make_async_remote_copy(
            src_ref=gref(ii, tile, s), dst_ref=gref(ii, tile, s), send_sem=ssem, recv_sem=rsem,
            device_id={"col": col, "row": row}, device_id_type=MESH)

    def zcopy(ii, tile, s, col):
        return gcopy(ii, tile, s, zs, grecv.at[ii // 2, tile, s], col, i)

    def ycopy(tile, s):
        return gcopy(i, tile, s, ys, grecv.at[i // 2, tile, s], z, iy)

    def pcopy(ii, tile, s):
        return gcopy(ii, tile, s, ps, precv.at[tile], z, ip)

    def done(ref, sem):
        pltpu.make_async_copy(ref, ref, sem).wait()

    def gwait(ii, tile, s):
        done(gref(ii, tile, s), grecv.at[ii // 2, tile, s])

    def loads(src, base, q, h):
        return pltpu.make_async_copy(src.at[halfrows(h), cols(q)], C.at[base + 2 * q + h], ld_sem.at[base // 2 + q])

    def each(n, body):
        def step(k, carry):
            body(k)
            return carry
        lax.fori_loop(0, n, step, 0)

    def start_loads(q):
        for h in range(2):
            loads(a_hbm, 0, q, h).start()
            loads(g_hbm, 2 * NQ, q, h).start()
    each(NQ, start_loads)

    barrier = pltpu.get_barrier_semaphore()
    me16 = z * 4 + i

    def knock(d):
        other = lax.rem(me16 + 1 + d, 16)
        pl.semaphore_signal(barrier, inc=1, device_id={"col": other // 4, "row": other % 4}, device_id_type=MESH)
    each(15, knock)
    pl.semaphore_wait(barrier, 15)

    def a_dst(zz, q):
        return AA.at[pos(zz) // 2, :, cols(pos(zz) % 2 * NQ + q)]

    def a_remote(q, h):
        return pltpu.make_async_remote_copy(
            src_ref=abuf.at[q, halfrows(h), :], dst_ref=a_dst(z, q),
            send_sem=asend, recv_sem=arecv, device_id={"col": 1 + h, "row": i}, device_id_type=MESH)

    def a_local(q, h):
        return pltpu.make_async_copy(abuf.at[q, halfrows(h), :], a_dst(z, q), arecv)

    def cast(src, base, q, dst):
        done(C.at[pl.ds(base + 2 * q, 2)], ld_sem.at[base // 2 + q])
        for h in range(2):
            gt[0, h * half:(h + 1) * half, :] = C[base + 2 * q + h].astype(BF16)
        put = pltpu.make_async_copy(gt.at[0, pl.ds(0, nb), :], dst, put_sem)
        put.start()
        put.wait()

    def hand_out(q):
        cast(a_hbm, 0, q, abuf.at[q])
        for h in range(2):
            @pl.when(z == 1 + h)
            def _():
                a_local(q, h).start()

            @pl.when(z != 1 + h)
            def _():
                a_remote(q, h).start()
        tile = z * NQ + q
        cast(g_hbm, 2 * NQ, q, gfull.at[tile, pl.ds(pl.multiple_of(pos(i) * nb, nb), nb), :])
        for s in range(NS):
            ycopy(tile, s).start()

            @pl.when(is_mid)
            def _():
                pcopy(i, tile, s).start()
    with jax.named_scope("hand_out"):
        each(NQ, hand_out)

    @pl.when(jnp.logical_not(is_mid))
    def _():
        def relay(q):
            tile = z * NQ + q
            for s in range(NS):
                zcopy(i, tile, s, mid).start()
            for s in range(NS):
                gwait(iy, tile, s)
                zcopy(iy, tile, s, mid).start()
        each(NQ, relay)

    def mtile(t):
        return jnp.where(t < NQ, omid * NQ + t, oend * NQ + t - NQ)

    def own_z(q):
        for s in range(NS):
            zcopy(i, z * NQ + q, s, omid).start()

    def y_pass(t):
        tm = mtile(t)
        for s in range(NS):
            gwait(iy, tm, s)
            pcopy(iy, tm, s).start()

    def z_pass(t):
        tm = mtile(t)
        for s in range(NS):
            gwait(i, tm, s)
            ycopy(tm, s).start()
            pcopy(i, tm, s).start()
        te = end * NQ + t // 2
        odd = t % 2

        @pl.when(odd == 0)
        def _():
            for s in range(NS):
                gwait(i, te, s)
                pcopy(i, te, s).start()

        @pl.when(odd == 1)
        def _():
            for s in range(NS):
                gwait(iy, te, s)
                pcopy(iy, te, s).start()

    def z_issue(t):
        @pl.when(t < NQ - 2)
        def _():
            own_z(t + 2)

        @pl.when(jnp.logical_or(jnp.logical_and(t >= NQ - 2, t <= 2 * NQ - 4), t == 2 * NQ - 2))
        def _():
            for s in range(NS):
                zcopy(i, end * NQ + jnp.minimum(t - NQ + 2, NQ - 1), s, omid).start()

    me8 = (z - 1) * 4 + i

    def half_load(tile, k, slot):
        return pltpu.make_async_copy(
            gfull.at[tile, pl.ds(pl.multiple_of(k * 2 * nb, 2 * nb), 2 * nb), :], gt.at[slot], tl_sem.at[slot])

    def blocks(body):
        def step(m, s):
            return body(pl.ds(pl.multiple_of(m * mb, mb), mb), s)
        return lax.fori_loop(0, half // mb, step, jnp.zeros((8, tw), F32))

    def fold(sq):
        return jnp.sum(sq.reshape(mb // 8, 8, tw), axis=0)

    def put_sum(it, tile, s):
        Sx[it, me8, :, cols(spos(tile))] = jnp.sum(s, axis=0, keepdims=True)

    def full(it, tile, dst):
        def block(r, s):
            acc = jnp.dot(AA[0, r, :], gt[0], preferred_element_type=F32)
            acc = acc + jnp.dot(AA[1, r, :], gt[1], preferred_element_type=F32)
            sq = acc * acc
            dst[r, :] = sq
            return s + fold(sq)
        put_sum(it, tile, blocks(block))

    def first_half(tile, slot):
        def block(r, s):
            C[tile, r, :] = jnp.dot(AA[2, r, :], gt[slot], preferred_element_type=F32)
            return s
        blocks(block)

    def second_half(tile, slot):
        def block(r, s):
            acc = C[tile, r, :] + jnp.dot(AA[1, r, :], gt[slot], preferred_element_type=F32)
            sq = acc * acc
            C[tile, r, :] = sq
            return s + fold(sq)
        put_sum(1, tile, blocks(block))

    def s_ref(part, src, n):
        if part < 2:
            return Sx.at[0, pl.ds(src, n), :, pl.ds(part * 2 * nb, 2 * nb)]
        return Sx.at[1, pl.ds(src, n)]

    def s_start(part):
        def send(d):
            other = lax.rem(me8 + d + 1, 8)
            pltpu.make_async_remote_copy(
                src_ref=s_ref(part, me8, 1), dst_ref=s_ref(part, me8, 1), send_sem=ss.at[part], recv_sem=sr.at[part],
                device_id={"col": 1 + other // 4, "row": other % 4}, device_id_type=MESH).start()
        each(7, send)

    def s_finish(part):
        done(s_ref(part, 0, 7), sr.at[part])
        lo, n, it = (part * 2 * nb, 2 * nb, 0) if part < 2 else (0, 4 * nb, 1)
        total = Sx[it, 0, :, lo:lo + n]
        for k in range(1, 8):
            total = total + Sx[it, k, :, lo:lo + n]
        scale[:, lo:lo + n] = float(order_n) / total
        done(s_ref(part, 0, 7), ss.at[part])

    def renorm(src, p, buf):
        fac = scale[:, cols(p)]

        def part(m):
            r = pl.ds(pl.multiple_of(m * mb, mb), mb)
            AA[buf, r, cols(p % (2 * NQ))] = (src[r, :] * fac).astype(BF16)
        each(half // mb, part)

    def b_number(tile):
        return jnp.where(tile // NQ == end, tile % NQ, NQ + tile % NQ)

    def m1_put(tile):
        k = b_number(tile)
        return pltpu.make_async_copy(C.at[tile], m1b.at[k], m1_sem.at[k])

    def m1_get(slot, k):
        return pltpu.make_async_copy(m1b.at[k], st.at[slot], st_sem.at[slot])

    def order3(k):
        j = k - NQ
        both = jnp.where(j % 2 == 0, omid, end) * NQ + j // 2
        return jnp.where(k < NQ, oend * NQ + k, jnp.where(k < 3 * NQ, both, mid * NQ + k - 3 * NQ))

    def c_remote(tile):
        q = tile % NQ
        return pltpu.make_async_remote_copy(
            src_ref=C.at[tile], dst_ref=chome.at[halfrows(z - 1), cols(q)],
            send_sem=csend, recv_sem=crecv,
            device_id={"col": tile // NQ, "row": i}, device_id_type=MESH)

    def c_local(tile):
        q = tile % NQ
        return pltpu.make_async_copy(C.at[tile], chome.at[halfrows(z - 1), cols(q)], crecv)

    def home_sum(k):
        zz, ii = k // 4, k % 4
        return pltpu.make_async_remote_copy(
            src_ref=Sx.at[2, me8, :, pl.ds(pl.multiple_of(pos(zz) * nb, nb), nb)], dst_ref=shome.at[me8],
            send_sem=hsend.at[k], recv_sem=hrecv,
            device_id={"col": zz, "row": ii}, device_id_type=MESH)

    def home_sum_local():
        return pltpu.make_async_copy(
            Sx.at[2, me8, :, pl.ds(pl.multiple_of(pos(z) * nb, nb), nb)], shome.at[me8], hrecv)

    @pl.when(is_mid)
    def _():
        own_z(0)
        own_z(1)

        def own_y(q):
            tile = z * NQ + q
            for s in range(NS):
                gwait(iy, tile, s)
                pcopy(iy, tile, s).start()
        with jax.named_scope("own_y"):
            each(NQ, own_y)

        with jax.named_scope("a_wait"):
            done(AA.at[pl.ds(0, 2)], arecv)

        def fetch(tile):
            done(gfull.at[tile, pl.ds(0, 2 * nb), :], precv.at[tile])
            for k in range(2):
                half_load(tile, k, k).start()
            for k in range(2):
                half_load(tile, k, k).wait()

        def own_cols(k):
            @pl.when(k == NQ // 2)
            def _():
                z_pass(0)
                z_issue(0)
            tile = mid * NQ + k
            fetch(tile)
            full(0, tile, C.at[tile])
        with jax.named_scope("own_cols"):
            each(NQ, own_cols)

        def extra(e):
            f = e - 2 * NQ - 6
            late = jnp.where(f % 3 == 2, end * NQ + 5 + f // 3, oend * NQ + 1 + 2 * (f // 3) + f % 3)
            b = jnp.where(e < 2 * NQ + 5, end * NQ + e - 2 * NQ, oend * NQ)
            return jnp.where(e < 2 * NQ, NQ + e, jnp.where(f < 0, b, late))

        def extras(lo, n):
            half_load(extra(lo), 0, 0).start()

            def part(u, carry):
                slot = u % 2
                te = extra(lo + u)

                @pl.when(u + 1 < n)
                def _():
                    half_load(extra(lo + u + 1), 0, 1 - slot).start()
                half_load(0, 0, slot).wait()

                @pl.when(lo + u >= 2 * NQ)
                def _():
                    m1_put(te).wait()
                first_half(te, slot)
                return carry
            with jax.named_scope("extra"):
                lax.fori_loop(0, n, part, 0)

        def slot_step(k):
            t = k + 1
            odd = t % 2

            @pl.when(t < 2 * NQ)
            def _():
                with jax.named_scope("z_pass"):
                    z_pass(t)

                @pl.when(t != NQ)
                def _():
                    z_issue(t)
            with jax.named_scope("y_pass"):
                y_pass(t - 1)

            @pl.when(t > NQ + 1)
            def _():
                extras(2 + 9 * ((t - 10) // 2) + 6 * odd, jnp.where(t == 2 * NQ, 2, 6 - 3 * odd))
            tile = mtile(t - 1)
            with jax.named_scope("fetch_m"):
                fetch(tile)
            full(0, tile, C.at[tile])

            @pl.when(t > NQ)
            def _():
                m1_put(tile).start()

            @pl.when(t == NQ)
            def _():
                s_start(0)
                z_issue(t)

            @pl.when(odd == 1)
            def _():
                te = end * NQ + t // 2
                with jax.named_scope("fetch_e"):
                    fetch(te)
                full(0, te, C.at[te])
                m1_put(te).start()

            @pl.when(t == NQ + 1)
            def _():
                with jax.named_scope("sums0"):
                    s_finish(0)

                def renorm_a(p):
                    zz = 1 + p // NQ
                    renorm(C.at[zz * NQ + p % NQ], p, 2)
                each(2 * NQ, renorm_a)
                extras(0, 2)
        each(2 * NQ, slot_step)
        extras(4 * NQ - 1, 1)
        half_load(0, 1, 0).start()
        half_load(NQ, 1, 1).start()
        def b_index(p):
            zz = jnp.where(p < NQ, 0, 3)
            return b_number(zz * NQ + p % NQ)

        for slot in range(2):
            m1_get(slot, b_index(slot)).start()
        s_start(1)
        with jax.named_scope("sums1"):
            s_finish(1)

        def renorm_b(p):
            slot = p % 2
            m1_get(slot, 0).wait()
            renorm(st.at[slot], 2 * NQ + p, 1)

            @pl.when(p + 2 < 2 * NQ)
            def _():
                m1_get(slot, b_index(p + 2)).start()
        with jax.named_scope("renorm_b"):
            each(2 * NQ, renorm_b)

        def order2(k):
            return (k % 4) * NQ + k // 4

        def second(k):
            slot = k % 2
            tile = order2(k)
            half_load(tile, 1, slot).wait()
            second_half(tile, slot)

            @pl.when(k + 2 < 4 * NQ)
            def _():
                half_load(order2(k + 2), 1, slot).start()
        with jax.named_scope("second"):
            each(4 * NQ, second)
        for k in range(2):
            half_load(order3(0), k, k).start()
        s_start(2)
        with jax.named_scope("sums2"):
            s_finish(2)

        def renorm_2(p):
            pz = p // NQ
            zz = jnp.where(pz == 2, 0, jnp.where(pz == 3, 3, pz + 1))
            renorm(C.at[zz * NQ + p % NQ], p, p // (2 * NQ))
        with jax.named_scope("renorm_2"):
            each(4 * NQ, renorm_2)

        def third(k):
            tile = order3(k)
            for u in range(2):
                half_load(tile, u, u).wait()
            full(2, tile, C.at[tile])

            @pl.when(k + 1 < 4 * NQ)
            def _():
                for u in range(2):
                    half_load(order3(k + 1), u, u).start()

            @pl.when(tile // NQ == z)
            def _():
                c_local(tile).start()

            @pl.when(tile // NQ != z)
            def _():
                c_remote(tile).start()
        with jax.named_scope("third"):
            each(4 * NQ, third)

        def send_sums(k):
            @pl.when(k == me16)
            def _():
                home_sum_local().start()

            @pl.when(k != me16)
            def _():
                home_sum(k).start()
        each(16, send_sums)

    with jax.named_scope("home_wait"):
        done(chome, crecv)
    done(shome, hrecv)
    done(gfull.at[pl.ds(0, 2 * NQ), pl.ds(0, nb), :], zs)

    @pl.when(jnp.logical_not(is_mid))
    def _():
        done(abuf, asend)
        done(gfull.at[pl.ds(0, NQ), pl.ds(0, nb), :], ys)

    @pl.when(is_mid)
    def _():
        done(abuf.at[:, pl.ds(0, half), :], asend)
        done(gfull.at[pl.ds(0, 3 * NQ), pl.ds(0, nb), :], ys)
        done(gfull.at[pl.ds(0, 2 * NQ)], ps)
        done(C.at[pl.ds(0, 3 * NQ)], csend)

        def drain(k):
            @pl.when(k != me16)
            def _():
                home_sum(k).wait_send()
        each(16, drain)


def solution(mesh):
    block_spec = P(("graph", "row"), "col")

    def device_step(init_blk, graph_blk):
        nb = init_blk.shape[1]
        n, tw = 4 * nb, nb // NQ
        mb = min(512, nb // 2)
        dma = pltpu.SemaphoreType.DMA
        any_spec = pl.BlockSpec(memory_space=pl.ANY)
        m_home, s_home, _, _, _ = pl.pallas_call(
            functools.partial(mcl_kernel, nb, mb),
            out_shape=(
                jax.ShapeDtypeStruct((nb, nb), F32),
                jax.ShapeDtypeStruct((8, 1, nb), F32),
                jax.ShapeDtypeStruct((4 * NQ, n, tw), BF16),
                jax.ShapeDtypeStruct((NQ, nb, tw), BF16),
                jax.ShapeDtypeStruct((2 * NQ, nb // 2, tw), F32),
            ),
            in_specs=[any_spec] * 2,
            out_specs=[any_spec] * 5,
            scratch_shapes=[
                pltpu.VMEM((3, nb // 2, 2 * nb), BF16),
                pltpu.VMEM((4 * NQ, nb // 2, tw), F32),
                pltpu.VMEM((2, 2 * nb, tw), BF16),
                pltpu.VMEM((2, nb // 2, tw), F32),
                pltpu.VMEM((3, 8, 1, n), F32),
                pltpu.VMEM((1, n), F32),
                dma((2 * NQ,)),
                dma(()),
                dma((2,)),
                dma((2,)),
                dma((2 * NQ,)),
                dma(()),
                dma(()),
                dma((2, 4 * NQ, NS)),
                dma((4 * NQ,)),
                dma(()),
                dma(()),
                dma(()),
                dma((3,)),
                dma((3,)),
                dma(()),
                dma(()),
                dma(()),
                dma((16,)),
            ],
            compiler_params=pltpu.CompilerParams(
                collective_id=0, has_side_effects=True, vmem_limit_bytes=67043328),
            name="mcl",
        )(init_blk, graph_blk)
        col_sum = jnp.sum(s_home, axis=(0, 1))
        return m_home * (n / col_sum)

    return jax.shard_map(device_step, mesh=mesh, in_specs=(block_spec, block_spec), out_specs=block_spec, check_vma=False)
```

```python
import functools

import jax
import jax.numpy as jnp
from jax import lax
from jax.experimental import pallas as pl
from jax.experimental.pallas import tpu as pltpu
from jax.sharding import PartitionSpec as P

ITERATIONS = 3
NQ = 8
NS = 2
MESH = pl.DeviceIdType.MESH
F32, BF16 = jnp.float32, jnp.bfloat16


def mcl_kernel(nb, mb, a_hbm, g_hbm, chome, shome, gfull, abuf, m1b, AA, C, gt, st, Sx, scale,
               ld_sem, put_sem, tl_sem, st_sem, m1_sem, arecv, asend, grecv, precv, zs, ys, ps, sr, ss, crecv, csend, hrecv, hsend):
    tw = nb // NQ
    half = nb // 2
    sub = nb // NS
    order_n = 4 * nb
    z, i = lax.axis_index("col"), lax.axis_index("row")
    y, c = i // 2, i % 2
    side = z // 2
    mid, omid, end, oend = 1 + side, 2 - side, 3 * side, 3 - 3 * side
    is_mid = z == mid
    iy, ip = (1 - y) * 2 + c, y * 2 + (1 - c)
    iyp = (1 - y) * 2 + (1 - c)

    def pos(zz):
        return jnp.where(zz == 0, 2, jnp.where(zz == 3, 3, zz - 1))

    def spos(tile):
        return pos(tile // NQ) * NQ + tile % NQ

    def cols(q):
        return pl.ds(pl.multiple_of(q * tw, tw), tw)

    def halfrows(h):
        return pl.ds(pl.multiple_of(h * half, half), half)

    def gref(ii, tile, s):
        return gfull.at[tile, pl.ds(pl.multiple_of(pos(ii) * nb + s * sub, sub), sub), :]

    def gcopy(ii, tile, s, ssem, rsem, col, row):
        return pltpu.make_async_remote_copy(
            src_ref=gref(ii, tile, s), dst_ref=gref(ii, tile, s), send_sem=ssem, recv_sem=rsem,
            device_id={"col": col, "row": row}, device_id_type=MESH)

    def zcopy(ii, tile, s, col):
        return gcopy(ii, tile, s, zs, grecv.at[ii // 2, tile, s], col, i)

    def ycopy(tile, s):
        return gcopy(i, tile, s, ys, grecv.at[i // 2, tile, s], z, iy)

    def pcopy(ii, tile, s):
        return gcopy(ii, tile, s, ps, precv.at[tile], z, ip)

    def done(ref, sem):
        pltpu.make_async_copy(ref, ref, sem).wait()

    def gwait(ii, tile, s):
        done(gref(ii, tile, s), grecv.at[ii // 2, tile, s])

    def loads(src, base, q, h):
        return pltpu.make_async_copy(src.at[halfrows(h), cols(q)], C.at[base + 2 * q + h], ld_sem.at[base // 2 + q])

    def each(n, body):
        def step(k, carry):
            body(k)
            return carry
        lax.fori_loop(0, n, step, 0)

    def start_loads(q):
        for h in range(2):
            loads(a_hbm, 0, q, h).start()
            loads(g_hbm, 2 * NQ, q, h).start()
    each(NQ, start_loads)

    barrier = pltpu.get_barrier_semaphore()
    me16 = z * 4 + i

    def knock(d):
        other = lax.rem(me16 + 1 + d, 16)
        pl.semaphore_signal(barrier, inc=1, device_id={"col": other // 4, "row": other % 4}, device_id_type=MESH)
    each(15, knock)
    pl.semaphore_wait(barrier, 15)

    def a_dst(zz, q):
        return AA.at[pos(zz) // 2, :, cols(pos(zz) % 2 * NQ + q)]

    def a_remote(q, h):
        return pltpu.make_async_remote_copy(
            src_ref=abuf.at[q, halfrows(h), :], dst_ref=a_dst(z, q),
            send_sem=asend, recv_sem=arecv, device_id={"col": 1 + h, "row": i}, device_id_type=MESH)

    def a_local(q, h):
        return pltpu.make_async_copy(abuf.at[q, halfrows(h), :], a_dst(z, q), arecv)

    def cast(src, base, q, dst):
        done(C.at[pl.ds(base + 2 * q, 2)], ld_sem.at[base // 2 + q])
        for h in range(2):
            gt[0, h * half:(h + 1) * half, :] = C[base + 2 * q + h].astype(BF16)
        put = pltpu.make_async_copy(gt.at[0, pl.ds(0, nb), :], dst, put_sem)
        put.start()
        put.wait()

    def hand_out(q):
        cast(a_hbm, 0, q, abuf.at[q])
        for h in range(2):
            @pl.when(z == 1 + h)
            def _():
                a_local(q, h).start()

            @pl.when(z != 1 + h)
            def _():
                a_remote(q, h).start()
        tile = z * NQ + q
        cast(g_hbm, 2 * NQ, q, gfull.at[tile, pl.ds(pl.multiple_of(pos(i) * nb, nb), nb), :])
        for s in range(NS):
            ycopy(tile, s).start()

            @pl.when(is_mid)
            def _():
                pcopy(i, tile, s).start()
    each(NQ, hand_out)

    @pl.when(jnp.logical_not(is_mid))
    def _():
        def relay(q):
            tile = z * NQ + q
            for s in range(NS):
                zcopy(i, tile, s, mid).start()
            for s in range(NS):
                gwait(iy, tile, s)
                zcopy(iy, tile, s, mid).start()
        each(NQ, relay)

    def mtile(t):
        return jnp.where(t < NQ, omid * NQ + t, oend * NQ + t - NQ)

    def own_z(q):
        for s in range(NS):
            zcopy(i, z * NQ + q, s, omid).start()

    def y_pass(t):
        tm = mtile(t)
        for s in range(NS):
            gwait(iy, tm, s)
            pcopy(iy, tm, s).start()

    def z_pass(t):
        tm = mtile(t)
        for s in range(NS):
            gwait(i, tm, s)
            ycopy(tm, s).start()
            pcopy(i, tm, s).start()
        te = end * NQ + t // 2
        odd = t % 2

        @pl.when(odd == 0)
        def _():
            for s in range(NS):
                gwait(i, te, s)
                pcopy(i, te, s).start()

        @pl.when(odd == 1)
        def _():
            for s in range(NS):
                gwait(iy, te, s)
                pcopy(iy, te, s).start()

    def z_issue(t):
        @pl.when(t < NQ - 2)
        def _():
            own_z(t + 2)

        @pl.when(jnp.logical_or(jnp.logical_and(t >= NQ - 2, t <= 2 * NQ - 4), t == 2 * NQ - 2))
        def _():
            for s in range(NS):
                zcopy(i, end * NQ + jnp.minimum(t - NQ + 2, NQ - 1), s, omid).start()

    me8 = (z - 1) * 4 + i

    def half_load(tile, k, slot):
        return pltpu.make_async_copy(
            gfull.at[tile, pl.ds(pl.multiple_of(k * 2 * nb, 2 * nb), 2 * nb), :], gt.at[slot], tl_sem.at[slot])

    def blocks(body):
        def step(m, s):
            return body(pl.ds(pl.multiple_of(m * mb, mb), mb), s)
        return lax.fori_loop(0, half // mb, step, jnp.zeros((8, tw), F32))

    def fold(sq):
        return jnp.sum(sq.reshape(mb // 8, 8, tw), axis=0)

    def put_sum(it, tile, s):
        Sx[it, me8, :, cols(spos(tile))] = jnp.sum(s, axis=0, keepdims=True)

    def full(it, tile, dst):
        def block(r, s):
            acc = jnp.dot(AA[0, r, :], gt[0], preferred_element_type=F32)
            acc = acc + jnp.dot(AA[1, r, :], gt[1], preferred_element_type=F32)
            sq = acc * acc
            dst[r, :] = sq
            return s + fold(sq)
        put_sum(it, tile, blocks(block))

    def first_half(tile, slot):
        def block(r, s):
            C[tile, r, :] = jnp.dot(AA[2, r, :], gt[slot], preferred_element_type=F32)
            return s
        blocks(block)

    def second_half(tile, slot):
        def block(r, s):
            acc = C[tile, r, :] + jnp.dot(AA[1, r, :], gt[slot], preferred_element_type=F32)
            sq = acc * acc
            C[tile, r, :] = sq
            return s + fold(sq)
        put_sum(1, tile, blocks(block))

    def s_ref(part, src, n):
        if part < 2:
            return Sx.at[0, pl.ds(src, n), :, pl.ds(part * 2 * nb, 2 * nb)]
        return Sx.at[1, pl.ds(src, n)]

    def s_start(part):
        def send(d):
            other = lax.rem(me8 + d + 1, 8)
            pltpu.make_async_remote_copy(
                src_ref=s_ref(part, me8, 1), dst_ref=s_ref(part, me8, 1), send_sem=ss.at[part], recv_sem=sr.at[part],
                device_id={"col": 1 + other // 4, "row": other % 4}, device_id_type=MESH).start()
        each(7, send)

    def s_finish(part):
        done(s_ref(part, 0, 7), sr.at[part])
        lo, n, it = (part * 2 * nb, 2 * nb, 0) if part < 2 else (0, 4 * nb, 1)
        total = Sx[it, 0, :, lo:lo + n]
        for k in range(1, 8):
            total = total + Sx[it, k, :, lo:lo + n]
        scale[:, lo:lo + n] = float(order_n) / total
        done(s_ref(part, 0, 7), ss.at[part])

    def renorm(src, p, buf):
        fac = scale[:, cols(p)]

        def part(m):
            r = pl.ds(pl.multiple_of(m * mb, mb), mb)
            AA[buf, r, cols(p % (2 * NQ))] = (src[r, :] * fac).astype(BF16)
        each(half // mb, part)

    def b_number(tile):
        return jnp.where(tile // NQ == end, tile % NQ, NQ + tile % NQ)

    def m1_put(tile):
        k = b_number(tile)
        return pltpu.make_async_copy(C.at[tile], m1b.at[k], m1_sem.at[k])

    def m1_get(slot, k):
        return pltpu.make_async_copy(m1b.at[k], st.at[slot], st_sem.at[slot])

    def order3(k):
        j = k - NQ
        both = jnp.where(j % 2 == 0, omid, end) * NQ + j // 2
        return jnp.where(k < NQ, oend * NQ + k, jnp.where(k < 3 * NQ, both, mid * NQ + k - 3 * NQ))

    def c_remote(tile):
        q = tile % NQ
        return pltpu.make_async_remote_copy(
            src_ref=C.at[tile], dst_ref=chome.at[halfrows(z - 1), cols(q)],
            send_sem=csend, recv_sem=crecv,
            device_id={"col": tile // NQ, "row": i}, device_id_type=MESH)

    def c_local(tile):
        q = tile % NQ
        return pltpu.make_async_copy(C.at[tile], chome.at[halfrows(z - 1), cols(q)], crecv)

    def home_sum(k):
        zz, ii = k // 4, k % 4
        return pltpu.make_async_remote_copy(
            src_ref=Sx.at[2, me8, :, pl.ds(pl.multiple_of(pos(zz) * nb, nb), nb)], dst_ref=shome.at[me8],
            send_sem=hsend.at[k], recv_sem=hrecv,
            device_id={"col": zz, "row": ii}, device_id_type=MESH)

    def home_sum_local():
        return pltpu.make_async_copy(
            Sx.at[2, me8, :, pl.ds(pl.multiple_of(pos(z) * nb, nb), nb)], shome.at[me8], hrecv)

    @pl.when(is_mid)
    def _():
        own_z(0)
        own_z(1)

        def own_y(q):
            tile = z * NQ + q
            for s in range(NS):
                gwait(iy, tile, s)
                pcopy(iy, tile, s).start()
        each(NQ, own_y)

        done(AA.at[pl.ds(0, 2)], arecv)

        def fetch(tile):
            done(gfull.at[tile, pl.ds(0, 2 * nb), :], precv.at[tile])
            for k in range(2):
                half_load(tile, k, k).start()
            for k in range(2):
                half_load(tile, k, k).wait()

        def own_cols(k):
            @pl.when(k == NQ // 2)
            def _():
                z_pass(0)
                z_issue(0)
            tile = mid * NQ + k
            fetch(tile)
            full(0, tile, C.at[tile])
        each(NQ, own_cols)

        def extra(e):
            f = e - 2 * NQ - 6
            late = jnp.where(f % 3 == 2, end * NQ + 5 + f // 3, oend * NQ + 1 + 2 * (f // 3) + f % 3)
            b = jnp.where(e < 2 * NQ + 5, end * NQ + e - 2 * NQ, oend * NQ)
            return jnp.where(e < 2 * NQ, NQ + e, jnp.where(f < 0, b, late))

        def extras(lo, n):
            half_load(extra(lo), 0, 0).start()

            def part(u, carry):
                slot = u % 2
                te = extra(lo + u)

                @pl.when(u + 1 < n)
                def _():
                    half_load(extra(lo + u + 1), 0, 1 - slot).start()
                half_load(0, 0, slot).wait()

                @pl.when(lo + u >= 2 * NQ)
                def _():
                    m1_put(te).wait()
                first_half(te, slot)
                return carry
            lax.fori_loop(0, n, part, 0)

        def slot_step(k):
            t = k + 1
            odd = t % 2

            @pl.when(t < 2 * NQ)
            def _():
                z_pass(t)

                @pl.when(t != NQ)
                def _():
                    z_issue(t)
            y_pass(t - 1)

            @pl.when(t > NQ + 1)
            def _():
                extras(2 + 9 * ((t - 10) // 2) + 6 * odd, jnp.where(t == 2 * NQ, 2, 6 - 3 * odd))
            tile = mtile(t - 1)
            fetch(tile)
            full(0, tile, C.at[tile])

            @pl.when(t > NQ)
            def _():
                m1_put(tile).start()

            @pl.when(t == NQ)
            def _():
                s_start(0)
                z_issue(t)

            @pl.when(odd == 1)
            def _():
                te = end * NQ + t // 2
                fetch(te)
                full(0, te, C.at[te])
                m1_put(te).start()

            @pl.when(t == NQ + 1)
            def _():
                s_finish(0)

                def renorm_a(p):
                    zz = 1 + p // NQ
                    renorm(C.at[zz * NQ + p % NQ], p, 2)
                each(2 * NQ, renorm_a)
                extras(0, 2)
        each(2 * NQ, slot_step)
        extras(4 * NQ - 1, 1)
        half_load(0, 1, 0).start()
        half_load(NQ, 1, 1).start()
        def b_index(p):
            zz = jnp.where(p < NQ, 0, 3)
            return b_number(zz * NQ + p % NQ)

        for slot in range(2):
            m1_get(slot, b_index(slot)).start()
        s_start(1)
        s_finish(1)

        def renorm_b(p):
            slot = p % 2
            m1_get(slot, 0).wait()
            renorm(st.at[slot], 2 * NQ + p, 1)

            @pl.when(p + 2 < 2 * NQ)
            def _():
                m1_get(slot, b_index(p + 2)).start()
        each(2 * NQ, renorm_b)

        def order2(k):
            return (k % 4) * NQ + k // 4

        def second(k):
            slot = k % 2
            tile = order2(k)
            half_load(tile, 1, slot).wait()
            second_half(tile, slot)

            @pl.when(k + 2 < 4 * NQ)
            def _():
                half_load(order2(k + 2), 1, slot).start()
        each(4 * NQ, second)
        for k in range(2):
            half_load(order3(0), k, k).start()
        s_start(2)
        s_finish(2)

        def renorm_2(p):
            pz = p // NQ
            zz = jnp.where(pz == 2, 0, jnp.where(pz == 3, 3, pz + 1))
            renorm(C.at[zz * NQ + p % NQ], p, p // (2 * NQ))
        each(4 * NQ, renorm_2)

        def third(k):
            tile = order3(k)
            for u in range(2):
                half_load(tile, u, u).wait()
            full(2, tile, C.at[tile])

            @pl.when(k + 1 < 4 * NQ)
            def _():
                for u in range(2):
                    half_load(order3(k + 1), u, u).start()

            @pl.when(tile // NQ == z)
            def _():
                c_local(tile).start()

            @pl.when(tile // NQ != z)
            def _():
                c_remote(tile).start()
        each(4 * NQ, third)

        def send_sums(k):
            @pl.when(k == me16)
            def _():
                home_sum_local().start()

            @pl.when(k != me16)
            def _():
                home_sum(k).start()
        each(16, send_sums)

    done(chome, crecv)
    done(shome, hrecv)
    done(gfull.at[pl.ds(0, 2 * NQ), pl.ds(0, nb), :], zs)

    @pl.when(jnp.logical_not(is_mid))
    def _():
        done(abuf, asend)
        done(gfull.at[pl.ds(0, NQ), pl.ds(0, nb), :], ys)

    @pl.when(is_mid)
    def _():
        done(abuf.at[:, pl.ds(0, half), :], asend)
        done(gfull.at[pl.ds(0, 3 * NQ), pl.ds(0, nb), :], ys)
        done(gfull.at[pl.ds(0, 2 * NQ)], ps)
        done(C.at[pl.ds(0, 3 * NQ)], csend)

        def drain(k):
            @pl.when(k != me16)
            def _():
                home_sum(k).wait_send()
        each(16, drain)


def solution(mesh):
    block_spec = P(("graph", "row"), "col")

    def device_step(init_blk, graph_blk):
        nb = init_blk.shape[1]
        n, tw = 4 * nb, nb // NQ
        mb = min(512, nb // 2)
        dma = pltpu.SemaphoreType.DMA
        any_spec = pl.BlockSpec(memory_space=pl.ANY)
        m_home, s_home, _, _, _ = pl.pallas_call(
            functools.partial(mcl_kernel, nb, mb),
            out_shape=(
                jax.ShapeDtypeStruct((nb, nb), F32),
                jax.ShapeDtypeStruct((8, 1, nb), F32),
                jax.ShapeDtypeStruct((4 * NQ, n, tw), BF16),
                jax.ShapeDtypeStruct((NQ, nb, tw), BF16),
                jax.ShapeDtypeStruct((2 * NQ, nb // 2, tw), F32),
            ),
            in_specs=[any_spec] * 2,
            out_specs=[any_spec] * 5,
            scratch_shapes=[
                pltpu.VMEM((3, nb // 2, 2 * nb), BF16),
                pltpu.VMEM((4 * NQ, nb // 2, tw), F32),
                pltpu.VMEM((2, 2 * nb, tw), BF16),
                pltpu.VMEM((2, nb // 2, tw), F32),
                pltpu.VMEM((3, 8, 1, n), F32),
                pltpu.VMEM((1, n), F32),
                dma((2 * NQ,)),
                dma(()),
                dma((2,)),
                dma((2,)),
                dma((2 * NQ,)),
                dma(()),
                dma(()),
                dma((2, 4 * NQ, NS)),
                dma((4 * NQ,)),
                dma(()),
                dma(()),
                dma(()),
                dma((3,)),
                dma((3,)),
                dma(()),
                dma(()),
                dma(()),
                dma((16,)),
            ],
            compiler_params=pltpu.CompilerParams(
                collective_id=0, has_side_effects=True, vmem_limit_bytes=67043328),
            name="mcl",
        )(init_blk, graph_blk)
        col_sum = jnp.sum(s_home, axis=(0, 1))
        return m_home * (n / col_sum)

    return jax.shard_map(device_step, mesh=mesh, in_specs=(block_spec, block_spec), out_specs=block_spec, check_vma=False)
```
